32 devices in a mesh: frag: 1 (over z), dev: 32 (over y, x, core).
Axes of the slice: x: 4, y: 4, z: 1, core: 2. Of those that a mesh axis runs over, the one named last changes fastest.
The devices are a block of a 4x4x8 slice.
Arguments:
- ao_ints: bfloat16 [160, 160, 160, 160], P(('frag', 'dev'))
- c_occ: bfloat16 [160, 32], P('frag')
- c_vir: bfloat16 [160, 104], P('frag')
Outputs:
- output 1: float32 [104, 104, 1024], P('frag', None, 'dev')
- output 2: float32 [32, 104, 3328], P('frag', None, 'dev')
All inputs are finite; a program needn't handle non-finite values.
Results may differ from the reference program's by a relative error of at most 0.001.
Values are sent between devices in bfloat16 or wider.
A program may use at most 768 MiB of HBM per device.

```python
import jax
import jax.numpy as jnp
from jax import lax

N_AO = 160
N_OCC = 32
N_VIR = 104


def setup_inputs(seed: int = 0, part: int = 0) -> dict:
    part_key = jax.random.fold_in(jax.random.key(seed), part)
    key_ints, key_occ, key_vir = jax.random.split(part_key, 3)
    row_keys = jax.random.split(key_ints, N_AO)

    def draw_row(row_key):
        return jax.random.normal(row_key, (N_AO, N_AO, N_AO), jnp.float32).astype(jnp.bfloat16)

    ao_ints = lax.map(draw_row, row_keys)
    coef_scale = N_AO ** -0.5
    c_occ = (jax.random.normal(key_occ, (N_AO, N_OCC), jnp.float32) * coef_scale).astype(jnp.bfloat16)
    c_vir = (jax.random.normal(key_vir, (N_AO, N_VIR), jnp.float32) * coef_scale).astype(jnp.bfloat16)
    return {'ao_ints': ao_ints, 'c_occ': c_occ, 'c_vir': c_vir}


def reference(ao_ints, c_occ, c_vir):
    occ32 = c_occ.astype(jnp.float32)
    vir32 = c_vir.astype(jnp.float32)

    def first_half(ao_row):
        quarter = jnp.einsum('qrs,rx->qsx', ao_row.astype(jnp.float32), occ32).astype(jnp.bfloat16)
        quarter32 = quarter.astype(jnp.float32)
        half_oo = jnp.einsum('qsx,sj->qxj', quarter32, occ32).astype(jnp.bfloat16)
        half_ov = jnp.einsum('qsx,sb->qxb', quarter32, vir32).astype(jnp.bfloat16)
        return half_oo, half_ov

    half_oo, half_ov = lax.map(first_half, ao_ints)
    half_oo = half_oo.reshape(N_AO, N_AO, N_OCC * N_OCC).astype(jnp.float32)
    half_ov = half_ov.reshape(N_AO, N_AO, N_OCC * N_VIR).astype(jnp.float32)
    mid_oo = jnp.einsum('pqm,qb->pbm', half_oo, vir32).astype(jnp.bfloat16).astype(jnp.float32)
    mid_ov = jnp.einsum('pqm,qa->pam', half_ov, vir32).astype(jnp.bfloat16).astype(jnp.float32)
    v_abij = jnp.einsum('pa,pbm->abm', vir32, mid_oo)
    v_iajb = jnp.einsum('pi,pam->iam', occ32, mid_ov)
    return v_abij, v_iajb
```

```python
import functools

import jax
import jax.numpy as jnp
from jax import lax
from jax.experimental import pallas as pl
from jax.experimental.pallas import tpu as pltpu
from jax.sharding import PartitionSpec as P

F32 = jnp.float32
BF16 = jnp.bfloat16
LANES = 128
TILE = 16
GROUP = 8


def _dot(lhs, rhs):
    return lax.dot_general(lhs, rhs, (((1,), (0,)), ((), ())), preferred_element_type=F32)


def _pieces(n_vir, moved):
    spare = LANES - n_vir
    slots = []
    for t in range(-(-moved * n_vir // spare)):
        runs = []
        col, end = t * spare, min((t + 1) * spare, moved * n_vir)
        at = n_vir
        while col < end:
            count = min(end, (col // n_vir + 1) * n_vir) - col
            runs.append((col // n_vir, col % n_vir, at, count))
            col, at = col + count, at + count
        slots.append(runs)
    return slots


def _kernel(n_dev, rows, n_ao, n_occ, n_vir, q_chunk, n_buf, pitch, keep,
            a_hbm, cot_ref, cv_ref, v1_ref, v2_ref,
            abuf, tb0, tb1, w2, ct, sb, rb, rep, wk, acc1, acc2, asem, ssem, rsem):
    me = lax.axis_index('dev')
    n_chunk = n_ao // q_chunk
    total = rows * n_chunk
    moved = (n_occ + n_vir) // GROUP - keep
    slots = _pieces(n_vir, moved)
    block_rows = keep * GROUP

    def fetch(chunk):
        slot = lax.rem(chunk, n_buf)
        return pltpu.make_async_copy(
            a_hbm.at[chunk // n_chunk, pl.ds(lax.rem(chunk, n_chunk) * q_chunk, q_chunk)],
            abuf.at[slot], asem.at[slot])

    for first in range(n_buf):
        fetch(jnp.int32(first)).start()

    barrier = pltpu.get_barrier_semaphore()

    @pl.loop(1, n_dev)
    def _(k):
        pl.semaphore_signal(barrier, inc=1, device_id={'dev': lax.rem(me + k, n_dev)},
                            device_id_type=pl.DeviceIdType.MESH)

    w2[...] = jnp.zeros_like(w2)
    w2[:n_ao, :n_vir] = cv_ref[...]
    w2[:n_ao, LANES:LANES + n_occ] = cot_ref[...].astype(F32).T.astype(BF16)
    ct[:n_occ, :] = cot_ref[...]
    ct[n_occ:, :] = cv_ref[...].astype(F32).T.astype(BF16)
    acc1[...] = jnp.zeros_like(acc1)
    acc2[...] = jnp.zeros_like(acc2)
    lane = lax.broadcasted_iota(jnp.int32, (GROUP, LANES), 1)

    pl.semaphore_wait(barrier, n_dev - 1)

    def send(row, x):
        return pltpu.make_async_remote_copy(
            src_ref=sb.at[row, x], dst_ref=rb.at[row, me],
            send_sem=ssem.at[row], recv_sem=rsem.at[row],
            device_id={'dev': x}, device_id_type=pl.DeviceIdType.MESH)

    @pl.loop(0, rows)
    def _(row):
        @pl.loop(0, n_chunk)
        def _(part):
            chunk = row * n_chunk + part
            slot = lax.rem(chunk, n_buf)
            fetch(chunk).wait()

            @pl.loop(0, q_chunk // 8)
            def _(block):
                for u in range(8):
                    q = block * 8 + u
                    t = _dot(cot_ref[...], abuf[slot, q])
                    at = pl.ds(part * q_chunk + q, n_occ, stride=pitch)
                    tb0[at, :] = t[:, :LANES]
                    tb1[at, :] = jnp.pad(t[:, LANES:], ((0, 0), (0, 2 * LANES - n_ao)))

            @pl.when(chunk + n_buf < total)
            def _():
                fetch(chunk + n_buf).start()

        @pl.loop(0, n_dev)
        def _(step):
            x = lax.rem(me + 1 + step, n_dev)
            at = pl.ds(pl.multiple_of(x * pitch, 8), n_ao)
            t = jnp.concatenate([tb0[at, :].astype(BF16), tb1[at, :].astype(BF16)], axis=1)
            h = _dot(t, w2[...])
            hov = h[:, :LANES].astype(BF16)
            hoo = h[:, LANES:LANES + n_occ].T.astype(BF16)
            gov = _dot(ct[n_occ:, :], hov)
            goo = _dot(hoo, w2[:n_ao, :LANES])
            groups = [goo[g * GROUP:(g + 1) * GROUP] for g in range(n_occ // GROUP)]
            groups += [gov[g * GROUP:(g + 1) * GROUP] for g in range(n_vir // GROUP)]
            out = []
            for t_, value in enumerate(groups[:keep]):
                for group, src, dst, _count in (slots[t_] if t_ < len(slots) else ()):
                    tail = groups[keep + group]
                    if (dst - src) % LANES:
                        tail = pltpu.roll(tail, (dst - src) % LANES, 1)
                    value = jnp.where(lane < dst, value, tail)
                out.append(value)
            sb[row, x] = jnp.concatenate(out, axis=0).astype(BF16)

            @pl.when(step > 0)
            def _():
                send(row, lax.rem(me + step, n_dev)).start()

        rb[row, me] = sb[row, me]

    ident = (lax.broadcasted_iota(jnp.int32, (TILE, n_dev * TILE), 1) % TILE
             == lax.broadcasted_iota(jnp.int32, (TILE, n_dev * TILE), 0))
    owner = (lax.broadcasted_iota(jnp.int32, (n_ao, n_dev * TILE), 1) // TILE) * rows
    place = lax.broadcasted_iota(jnp.int32, (n_ao, n_dev * TILE), 0)
    n_tile = block_rows // TILE
    oo_rows = n_occ * TILE

    @pl.loop(0, rows)
    def _(row):
        pick = jnp.where(place == owner + row, 1.0, 0.0).astype(BF16)
        rep[...] = _dot(ct[...], pick)

        @pl.loop(0, (n_occ + n_vir) // 8)
        def _(block):
            for u in range(8):
                i = block * 8 + u
                value = jnp.where(ident, rep[pl.ds(i, 1), :], 0.0).astype(BF16)
                wk[pl.ds(pl.multiple_of(i * TILE, TILE), TILE), :] = value

        pltpu.make_async_copy(rb.at[row, pl.ds(0, n_dev - 1)], rb.at[row, pl.ds(0, n_dev - 1)],
                              rsem.at[row]).wait()

        def tiles(first, count):
            parts = [rb[row, :, t * TILE:(t + 1) * TILE, :].reshape(n_dev * TILE, LANES)
                     for t in range(first, first + count)]
            return parts[0] if count == 1 else jnp.concatenate(parts, axis=1)

        for first in range(0, n_tile, 2):
            count = min(2, n_tile - first)
            out = _dot(wk[:oo_rows, :], tiles(first, count))
            for c in range(count):
                at = slice((first + c) * TILE, (first + c + 1) * TILE)
                acc2[:, at, :] += out[:, c * LANES:(c + 1) * LANES].reshape(n_occ, TILE, LANES)

        n_block = n_vir // GROUP
        rhs = tiles(0, n_occ // TILE)

        @pl.loop(0, n_block)
        def _(block):
            at = pl.ds(pl.multiple_of(oo_rows + block * (GROUP * TILE), TILE), GROUP * TILE)
            out = _dot(wk[at, :], rhs)
            for c in range(n_occ // TILE):
                acc1[pl.ds(block * GROUP, GROUP), c * TILE:(c + 1) * TILE, :] += (
                    out[:, c * LANES:(c + 1) * LANES].reshape(GROUP, TILE, LANES))

    v1_ref[...] = acc1[:, :, :n_vir]
    head = n_vir // GROUP - moved
    v2_ref[:, :head * GROUP, :] = acc2[:, n_occ:n_occ + head * GROUP, :n_vir]

    @pl.loop(0, n_occ)
    def _(i):
        for group in range(moved):
            value = None
            for t, runs in enumerate(slots):
                for g, src, dst, _count in runs:
                    if g == group:
                        piece = acc2[i, t * GROUP:(t + 1) * GROUP, :]
                        if (src - dst) % LANES:
                            piece = pltpu.roll(piece, (src - dst) % LANES, 1)
                        value = piece if value is None else jnp.where(lane < src, value, piece)
            v2_ref[i, (head + group) * GROUP:(head + group + 1) * GROUP, :] = value[:, :n_vir]

    for row in range(rows):
        pltpu.make_async_copy(sb.at[row, pl.ds(0, n_dev - 1)], sb.at[row, pl.ds(0, n_dev - 1)],
                              ssem.at[row]).wait()


def solution(mesh):
    n_dev = mesh.shape['dev']

    def local_part(ao_rows, c_occ, c_vir):
        rows, n_ao = ao_rows.shape[:2]
        n_occ, n_vir = c_occ.shape[1], c_vir.shape[1]
        assert n_occ == n_dev
        q_chunk, n_buf, pitch = 32, 3, n_ao + 8
        keep = 14
        block_rows = keep * GROUP
        n_mo = n_occ + n_vir
        v1, v2 = pl.pallas_call(
            functools.partial(_kernel, n_dev, rows, n_ao, n_occ, n_vir, q_chunk, n_buf, pitch, keep),
            out_shape=(jax.ShapeDtypeStruct((n_vir, n_occ, n_vir), F32),
                       jax.ShapeDtypeStruct((n_occ, n_vir, n_vir), F32)),
            in_specs=[pl.BlockSpec(memory_space=pl.ANY),
                      pl.BlockSpec(memory_space=pltpu.VMEM),
                      pl.BlockSpec(memory_space=pltpu.VMEM)],
            out_specs=(pl.BlockSpec(memory_space=pltpu.VMEM), pl.BlockSpec(memory_space=pltpu.VMEM)),
            scratch_shapes=[
                pltpu.VMEM((n_buf, q_chunk, n_ao, n_ao), BF16),
                pltpu.VMEM((n_occ * pitch, LANES), F32),
                pltpu.VMEM((n_occ * pitch, LANES), F32),
                pltpu.VMEM((2 * LANES, 2 * LANES), BF16),
                pltpu.VMEM((n_mo, n_ao), BF16),
                pltpu.VMEM((rows, n_dev, block_rows, LANES), BF16),
                pltpu.VMEM((rows, n_dev, block_rows, LANES), BF16),
                pltpu.VMEM((n_mo, n_dev * TILE), F32),
                pltpu.VMEM((n_mo * TILE, n_dev * TILE), BF16),
                pltpu.VMEM((n_vir, n_occ, LANES), F32),
                pltpu.VMEM((n_occ, block_rows, LANES), F32),
                pltpu.SemaphoreType.DMA((n_buf,)),
                pltpu.SemaphoreType.DMA((rows,)),
                pltpu.SemaphoreType.DMA((rows,)),
            ],
            compiler_params=pltpu.CompilerParams(collective_id=0, has_side_effects=True,
                                                 vmem_limit_bytes=60 * 1024 * 1024),
        )(ao_rows, c_occ.T, c_vir)
        return v1.transpose(0, 2, 1), v2

    return jax.shard_map(local_part, mesh=mesh,
                         in_specs=(P(('frag', 'dev')), P('frag'), P('frag')),
                         out_specs=(P('frag', None, 'dev'), P('frag', None, 'dev')),
                         check_vma=False)
```

```python
import functools

import jax
import jax.numpy as jnp
from jax import lax
from jax.experimental import pallas as pl
from jax.experimental.pallas import tpu as pltpu
from jax.sharding import PartitionSpec as P

F32 = jnp.float32
BF16 = jnp.bfloat16
LANES = 128
TILE = 16
GROUP = 8


def _dot(lhs, rhs):
    return lax.dot_general(lhs, rhs, (((1,), (0,)), ((), ())), preferred_element_type=F32)


def _pieces(n_vir, moved):
    spare = LANES - n_vir
    slots = []
    for t in range(-(-moved * n_vir // spare)):
        runs = []
        col, end = t * spare, min((t + 1) * spare, moved * n_vir)
        at = n_vir
        while col < end:
            count = min(end, (col // n_vir + 1) * n_vir) - col
            runs.append((col // n_vir, col % n_vir, at, count))
            col, at = col + count, at + count
        slots.append(runs)
    return slots


def _kernel(n_dev, rows, n_ao, n_occ, n_vir, q_chunk, n_buf, pitch, keep, unroll,
            a_hbm, cot_ref, cv_ref, v1_ref, v2_ref,
            abuf, tb0, tb1, w2, ct, hov0, hov1, hoo0, hoo1, sb, rb, rep, wk, acc1, acc2, asem, ssem, rsem):
    me = lax.axis_index('dev')
    hov, hoo = (hov0, hov1), (hoo0, hoo1)
    n_chunk = n_ao // q_chunk
    total = rows * n_chunk
    moved = (n_occ + n_vir) // GROUP - keep
    slots = _pieces(n_vir, moved)
    block_rows = keep * GROUP

    def fetch(chunk):
        slot = lax.rem(chunk, n_buf)
        return pltpu.make_async_copy(
            a_hbm.at[chunk // n_chunk, pl.ds(lax.rem(chunk, n_chunk) * q_chunk, q_chunk)],
            abuf.at[slot], asem.at[slot])

    for first in range(n_buf):
        fetch(jnp.int32(first)).start()

    barrier = pltpu.get_barrier_semaphore()

    @pl.loop(1, n_dev)
    def _(k):
        pl.semaphore_signal(barrier, inc=1, device_id={'dev': lax.rem(me + k, n_dev)},
                            device_id_type=pl.DeviceIdType.MESH)

    w2[...] = jnp.zeros_like(w2)
    w2[:n_ao, :n_vir] = cv_ref[...]
    w2[:n_ao, LANES:LANES + n_occ] = cot_ref[...].astype(F32).T.astype(BF16)
    ct[:n_occ, :] = cot_ref[...]
    ct[n_occ:, :] = cv_ref[...].astype(F32).T.astype(BF16)
    acc1[...] = jnp.zeros_like(acc1)
    acc2[...] = jnp.zeros_like(acc2)
    lane = lax.broadcasted_iota(jnp.int32, (GROUP, LANES), 1)

    pl.semaphore_wait(barrier, n_dev - 1)

    def send(row, x):
        return pltpu.make_async_remote_copy(
            src_ref=sb.at[row, x], dst_ref=rb.at[row, me],
            send_sem=ssem.at[row], recv_sem=rsem.at[row],
            device_id={'dev': x}, device_id_type=pl.DeviceIdType.MESH)

    @pl.loop(0, rows)
    def _(row):
        @pl.loop(0, n_chunk)
        def _(part):
            chunk = row * n_chunk + part
            slot = lax.rem(chunk, n_buf)
            fetch(chunk).wait()

            for q in range(q_chunk):
                t = _dot(cot_ref[...], abuf[slot, q])
                at = pl.ds(part * q_chunk + q, n_occ, stride=pitch)
                tb0[at, :] = t[:, :LANES]
                tb1[at, :] = jnp.pad(t[:, LANES:], ((0, 0), (0, 2 * LANES - n_ao)))

            @pl.when(chunk + n_buf < total)
            def _():
                fetch(chunk + n_buf).start()

        def owner_of(step):
            return lax.rem(me + 1 + step, n_dev)

        def half(group):
            parts = []
            for u in range(unroll):
                at = pl.ds(pl.multiple_of(owner_of(group * unroll + u) * pitch, 8), n_ao)
                parts.append(jnp.concatenate([tb0[at, :].astype(BF16), tb1[at, :].astype(BF16)], axis=1))
            h = _dot(jnp.concatenate(parts, axis=0), w2[...])
            for u in range(unroll):
                at = slice(u * n_ao, (u + 1) * n_ao)
                hov[group % 2][u] = h[at, :LANES].astype(BF16)
                hoo[group % 2][u * n_occ:(u + 1) * n_occ, :] = h[at, LANES:LANES + n_occ].T.astype(BF16)

        def full(group):
            goo = _dot(hoo[group % 2][...], w2[:n_ao, :LANES])
            for u in range(0, unroll, 2):
                pair = _dot(ct[n_occ:, :], jnp.concatenate([hov[group % 2][u], hov[group % 2][u + 1]], axis=1))
                for v in range(2):
                    gov = pair[:, v * LANES:(v + 1) * LANES]
                    first = (u + v) * n_occ
                    groups = [goo[first + g * GROUP:first + (g + 1) * GROUP] for g in range(n_occ // GROUP)]
                    groups += [gov[g * GROUP:(g + 1) * GROUP] for g in range(n_vir // GROUP)]
                    out = []
                    for t_, value in enumerate(groups[:keep]):
                        for part, src, dst, _count in (slots[t_] if t_ < len(slots) else ()):
                            tail = groups[keep + part]
                            if (dst - src) % LANES:
                                tail = pltpu.roll(tail, (dst - src) % LANES, 1)
                            value = jnp.where(lane < dst, value, tail)
                        out.append(value)
                    sb[row, owner_of(group * unroll + u + v)] = jnp.concatenate(out, axis=0).astype(BF16)

        n_group = n_dev // unroll
        half(0)
        for group in range(n_group):
            if group + 1 < n_group:
                half(group + 1)
            full(group)
            if group:
                for u in range(unroll):
                    send(row, owner_of((group - 1) * unroll + u)).start()
        rb[row, me] = sb[row, me]
        for u in range(unroll - 1):
            send(row, owner_of((n_group - 1) * unroll + u)).start()

    ident = (lax.broadcasted_iota(jnp.int32, (TILE, n_dev * TILE), 1) % TILE
             == lax.broadcasted_iota(jnp.int32, (TILE, n_dev * TILE), 0))
    owner = (lax.broadcasted_iota(jnp.int32, (n_ao, n_dev * TILE), 1) // TILE) * rows
    place = lax.broadcasted_iota(jnp.int32, (n_ao, n_dev * TILE), 0)
    n_tile = block_rows // TILE
    oo_rows = n_occ * TILE

    @pl.loop(0, rows)
    def _(row):
        pick = jnp.where(place == owner + row, 1.0, 0.0).astype(BF16)
        rep[...] = _dot(ct[...], pick)

        @pl.loop(0, (n_occ + n_vir) // 8)
        def _(block):
            for u in range(8):
                i = block * 8 + u
                value = jnp.where(ident, rep[pl.ds(i, 1), :], 0.0).astype(BF16)
                wk[pl.ds(pl.multiple_of(i * TILE, TILE), TILE), :] = value

        pltpu.make_async_copy(rb.at[row, pl.ds(0, n_dev - 1)], rb.at[row, pl.ds(0, n_dev - 1)],
                              rsem.at[row]).wait()

        def tiles(first, count):
            parts = [rb[row, :, t * TILE:(t + 1) * TILE, :].reshape(n_dev * TILE, LANES)
                     for t in range(first, first + count)]
            return parts[0] if count == 1 else jnp.concatenate(parts, axis=1)

        for first in range(0, n_tile, 2):
            count = min(2, n_tile - first)
            out = _dot(wk[:oo_rows, :], tiles(first, count))
            for c in range(count):
                at = slice((first + c) * TILE, (first + c + 1) * TILE)
                acc2[:, at, :] += out[:, c * LANES:(c + 1) * LANES].reshape(n_occ, TILE, LANES)

        n_block = 4
        span = n_vir // n_block
        rhs = tiles(0, n_occ // TILE)

        @pl.loop(0, n_block)
        def _(block):
            at = pl.ds(pl.multiple_of(oo_rows + block * (span * TILE), TILE), span * TILE)
            out = _dot(wk[at, :], rhs)
            for c in range(n_occ // TILE):
                acc1[pl.ds(block * span, span), c * TILE:(c + 1) * TILE, :] += (
                    out[:, c * LANES:(c + 1) * LANES].reshape(span, TILE, LANES))

    v1_ref[...] = acc1[:, :, :n_vir]
    head = n_vir // GROUP - moved
    v2_ref[:, :head * GROUP, :] = acc2[:, n_occ:n_occ + head * GROUP, :n_vir]

    @pl.loop(0, n_occ)
    def _(i):
        for group in range(moved):
            value = None
            for t, runs in enumerate(slots):
                for g, src, dst, _count in runs:
                    if g == group:
                        piece = acc2[i, t * GROUP:(t + 1) * GROUP, :]
                        if (src - dst) % LANES:
                            piece = pltpu.roll(piece, (src - dst) % LANES, 1)
                        value = piece if value is None else jnp.where(lane < src, value, piece)
            v2_ref[i, (head + group) * GROUP:(head + group + 1) * GROUP, :] = value[:, :n_vir]

    for row in range(rows):
        pltpu.make_async_copy(sb.at[row, pl.ds(0, n_dev - 1)], sb.at[row, pl.ds(0, n_dev - 1)],
                              ssem.at[row]).wait()


def solution(mesh):
    n_dev = mesh.shape['dev']

    def local_part(ao_rows, c_occ, c_vir):
        rows, n_ao = ao_rows.shape[:2]
        n_occ, n_vir = c_occ.shape[1], c_vir.shape[1]
        assert n_occ == n_dev
        q_chunk, n_buf, pitch = 32, 3, n_ao + 8
        keep, unroll = 14, 8
        block_rows = keep * GROUP
        n_mo = n_occ + n_vir
        v1, v2 = pl.pallas_call(
            functools.partial(_kernel, n_dev, rows, n_ao, n_occ, n_vir, q_chunk, n_buf, pitch, keep, unroll),
            out_shape=(jax.ShapeDtypeStruct((n_vir, n_occ, n_vir), F32),
                       jax.ShapeDtypeStruct((n_occ, n_vir, n_vir), F32)),
            in_specs=[pl.BlockSpec(memory_space=pl.ANY),
                      pl.BlockSpec(memory_space=pltpu.VMEM),
                      pl.BlockSpec(memory_space=pltpu.VMEM)],
            out_specs=(pl.BlockSpec(memory_space=pltpu.VMEM), pl.BlockSpec(memory_space=pltpu.VMEM)),
            scratch_shapes=[
                pltpu.VMEM((n_buf, q_chunk, n_ao, n_ao), BF16),
                pltpu.VMEM((n_occ * pitch, LANES), F32),
                pltpu.VMEM((n_occ * pitch, LANES), F32),
                pltpu.VMEM((2 * LANES, 2 * LANES), BF16),
                pltpu.VMEM((n_mo, n_ao), BF16),
                pltpu.VMEM((unroll, n_ao, LANES), BF16),
                pltpu.VMEM((unroll, n_ao, LANES), BF16),
                pltpu.VMEM((unroll * n_occ, n_ao), BF16),
                pltpu.VMEM((unroll * n_occ, n_ao), BF16),
                pltpu.VMEM((rows, n_dev, block_rows, LANES), BF16),
                pltpu.VMEM((rows, n_dev, block_rows, LANES), BF16),
                pltpu.VMEM((n_mo, n_dev * TILE), F32),
                pltpu.VMEM((n_mo * TILE, n_dev * TILE), BF16),
                pltpu.VMEM((n_vir, n_occ, LANES), F32),
                pltpu.VMEM((n_occ, block_rows, LANES), F32),
                pltpu.SemaphoreType.DMA((n_buf,)),
                pltpu.SemaphoreType.DMA((rows,)),
                pltpu.SemaphoreType.DMA((rows,)),
            ],
            compiler_params=pltpu.CompilerParams(collective_id=0, has_side_effects=True,
                                                 vmem_limit_bytes=60 * 1024 * 1024),
        )(ao_rows, c_occ.T, c_vir)
        return v1.transpose(0, 2, 1), v2

    return jax.shard_map(local_part, mesh=mesh,
                         in_specs=(P(('frag', 'dev')), P('frag'), P('frag')),
                         out_specs=(P('frag', None, 'dev'), P('frag', None, 'dev')),
                         check_vma=False)
```

```python
import functools
import math

import jax
import jax.numpy as jnp
from jax import lax
from jax.experimental import pallas as pl
from jax.experimental.pallas import tpu as pltpu
from jax.sharding import PartitionSpec as P

F32 = jnp.float32
BF16 = jnp.bfloat16
LANES = 128
TILE = 16
GROUP = 8


def _dot(lhs, rhs):
    return lax.dot_general(lhs, rhs, (((1,), (0,)), ((), ())), preferred_element_type=F32)


def _pieces(n_vir, moved):
    spare = LANES - n_vir
    slots = []
    for t in range(-(-moved * n_vir // spare)):
        runs = []
        col, end = t * spare, min((t + 1) * spare, moved * n_vir)
        at = n_vir
        while col < end:
            count = min(end, (col // n_vir + 1) * n_vir) - col
            runs.append((col // n_vir, col % n_vir, at, count))
            col, at = col + count, at + count
        slots.append(runs)
    return slots


def _order(side):
    def hops(d):
        return min(d, side - d)

    left = {(dx, dy) for dx in range(side) for dy in range(side)}
    chips = []
    for dx, dy in sorted(left, key=lambda c: (-(hops(c[0]) > 0) - (hops(c[1]) > 0),
                                              abs(hops(c[0]) - hops(c[1])), hops(c[0]), c)):
        for chip in ((dx, dy), (-dx % side, -dy % side), (dy, -dx % side), (-dy % side, dx)):
            if chip in left:
                left.remove(chip)
                chips.append(chip)
    return [(dx, dy, other) for dx, dy in chips for other in (1, 0)]


def _kernel(n_dev, rows, n_ao, n_occ, n_vir, q_chunk, n_buf, pitch, keep, unroll,
            a_hbm, cot_ref, cv_ref, acc1, acc2,
            abuf, tb0, tb1, w2, ct, hov0, hov1, hoo0, hoo1, sb, rb, rep, wk, asem, ssem, rsem):
    me = lax.axis_index('dev')
    hov, hoo = (hov0, hov1), (hoo0, hoo1)
    side = math.isqrt(n_dev // 2)
    core, cx, cy = lax.rem(me, 2), lax.rem(me // 2, side), me // (2 * side)
    sign = 1 - 2 * core
    order = _order(side)
    n_chunk = n_ao // q_chunk
    total = rows * n_chunk
    moved = (n_occ + n_vir) // GROUP - keep
    slots = _pieces(n_vir, moved)
    block_rows = keep * GROUP

    def fetch(chunk):
        slot = lax.rem(chunk, n_buf)
        return pltpu.make_async_copy(
            a_hbm.at[chunk // n_chunk, pl.ds(lax.rem(chunk, n_chunk) * q_chunk, q_chunk)],
            abuf.at[slot], asem.at[slot])

    for first in range(n_buf):
        fetch(jnp.int32(first)).start()

    barrier = pltpu.get_barrier_semaphore()

    @pl.loop(1, n_dev)
    def _(k):
        pl.semaphore_signal(barrier, inc=1, device_id={'dev': lax.rem(me + k, n_dev)},
                            device_id_type=pl.DeviceIdType.MESH)

    w2[...] = jnp.zeros_like(w2)
    w2[:n_ao, :n_vir] = cv_ref[...]
    w2[:n_ao, LANES:LANES + n_occ] = cot_ref[...].astype(F32).T.astype(BF16)
    ct[:n_occ, :] = cot_ref[...]
    ct[n_occ:, :] = cv_ref[...].astype(F32).T.astype(BF16)
    acc1[...] = jnp.zeros_like(acc1)
    acc2[...] = jnp.zeros_like(acc2)
    lane = lax.broadcasted_iota(jnp.int32, (GROUP, LANES), 1)

    pl.semaphore_wait(barrier, n_dev - 1)

    def send(row, x):
        return pltpu.make_async_remote_copy(
            src_ref=sb.at[row, x], dst_ref=rb.at[row, me],
            send_sem=ssem.at[row], recv_sem=rsem.at[row],
            device_id={'dev': x}, device_id_type=pl.DeviceIdType.MESH)

    @pl.loop(0, rows)
    def _(row):
        @pl.loop(0, n_chunk)
        def _(part):
            chunk = row * n_chunk + part
            slot = lax.rem(chunk, n_buf)
            fetch(chunk).wait()

            for q in range(q_chunk):
                t = _dot(cot_ref[...], abuf[slot, q])
                at = pl.ds(part * q_chunk + q, n_occ, stride=pitch)
                tb0[at, :] = t[:, :LANES]
                tb1[at, :] = jnp.pad(t[:, LANES:], ((0, 0), (0, 2 * LANES - n_ao)))

            @pl.when(chunk + n_buf < total)
            def _():
                fetch(chunk + n_buf).start()

        def owner_of(step):
            dx, dy, other = order[step]
            return ((lax.rem(cy + dy * sign + side, side) * side + lax.rem(cx + dx * sign + side, side)) * 2
                    + lax.rem(core + other, 2))

        def half(group):
            parts = []
            for u in range(unroll):
                at = pl.ds(pl.multiple_of(owner_of(group * unroll + u) * pitch, 8), n_ao)
                parts.append(jnp.concatenate([tb0[at, :].astype(BF16), tb1[at, :].astype(BF16)], axis=1))
            h = _dot(jnp.concatenate(parts, axis=0), w2[...])
            for u in range(unroll):
                at = slice(u * n_ao, (u + 1) * n_ao)
                hov[group % 2][u] = h[at, :LANES].astype(BF16)
                hoo[group % 2][u * n_occ:(u + 1) * n_occ, :] = h[at, LANES:LANES + n_occ].T.astype(BF16)

        def full(group):
            goo = _dot(hoo[group % 2][...], w2[:n_ao, :LANES])
            for u in range(0, unroll, 2):
                pair = _dot(ct[n_occ:, :], jnp.concatenate([hov[group % 2][u], hov[group % 2][u + 1]], axis=1))
                for v in range(2):
                    gov = pair[:, v * LANES:(v + 1) * LANES]
                    first = (u + v) * n_occ
                    groups = [goo[first + g * GROUP:first + (g + 1) * GROUP] for g in range(n_occ // GROUP)]
                    groups += [gov[g * GROUP:(g + 1) * GROUP] for g in range(n_vir // GROUP)]
                    out = []
                    for t_, value in enumerate(groups[:keep]):
                        for part, src, dst, _count in (slots[t_] if t_ < len(slots) else ()):
                            tail = groups[keep + part]
                            if (dst - src) % LANES:
                                tail = pltpu.roll(tail, (dst - src) % LANES, 1)
                            value = jnp.where(lane < dst, value, tail)
                        out.append(value)
                    sb[row, owner_of(group * unroll + u + v)] = jnp.concatenate(out, axis=0).astype(BF16)

        n_group = n_dev // unroll
        half(0)
        for group in range(n_group):
            if group + 1 < n_group:
                half(group + 1)
            full(group)
            if group:
                for u in range(unroll):
                    send(row, owner_of((group - 1) * unroll + u)).start()
        rb[row, me] = sb[row, me]
        for u in range(unroll - 1):
            send(row, owner_of((n_group - 1) * unroll + u)).start()

    ident = (lax.broadcasted_iota(jnp.int32, (TILE, n_dev * TILE), 1) % TILE
             == lax.broadcasted_iota(jnp.int32, (TILE, n_dev * TILE), 0))
    owner = (lax.broadcasted_iota(jnp.int32, (n_ao, n_dev * TILE), 1) // TILE) * rows
    place = lax.broadcasted_iota(jnp.int32, (n_ao, n_dev * TILE), 0)
    n_tile = block_rows // TILE
    oo_rows = n_occ * TILE

    @pl.loop(0, rows)
    def _(row):
        pick = jnp.where(place == owner + row, 1.0, 0.0).astype(BF16)
        rep[...] = _dot(ct[...], pick)

        @pl.loop(0, (n_occ + n_vir) // 8)
        def _(block):
            for u in range(8):
                i = block * 8 + u
                value = jnp.where(ident, rep[pl.ds(i, 1), :], 0.0).astype(BF16)
                wk[pl.ds(pl.multiple_of(i * TILE, TILE), TILE), :] = value

        pltpu.make_async_copy(rb.at[row, pl.ds(0, n_dev - 1)], rb.at[row, pl.ds(0, n_dev - 1)],
                              rsem.at[row]).wait()

        def tiles(first, count):
            parts = [rb[row, :, t * TILE:(t + 1) * TILE, :].reshape(n_dev * TILE, LANES)
                     for t in range(first, first + count)]
            return parts[0] if count == 1 else jnp.concatenate(parts, axis=1)

        for first in range(0, n_tile, 2):
            count = min(2, n_tile - first)
            out = _dot(wk[:oo_rows, :], tiles(first, count))
            for c in range(count):
                at = slice((first + c) * TILE, (first + c + 1) * TILE)
                acc2[:, at, :] += out[:, c * LANES:(c + 1) * LANES].reshape(n_occ, TILE, LANES)

        n_block = 4
        span = n_vir // n_block
        rhs = tiles(0, n_occ // TILE)

        @pl.loop(0, n_block)
        def _(block):
            at = pl.ds(pl.multiple_of(oo_rows + block * (span * TILE), TILE), span * TILE)
            out = _dot(wk[at, :], rhs)
            for c in range(n_occ // TILE):
                acc1[pl.ds(block * span, span), c * TILE:(c + 1) * TILE, :] += (
                    out[:, c * LANES:c * LANES + n_vir].reshape(span, TILE, n_vir))

    for row in range(rows):
        pltpu.make_async_copy(sb.at[row, pl.ds(0, n_dev - 1)], sb.at[row, pl.ds(0, n_dev - 1)],
                              ssem.at[row]).wait()


def _unpack(n_occ, n_vir, keep, acc1, acc2, v1_ref, v2_ref, v2, sem):
    moved = (n_occ + n_vir) // GROUP - keep
    head = n_vir // GROUP - moved
    slots = _pieces(n_vir, moved)
    lane = lax.broadcasted_iota(jnp.int32, (GROUP, LANES), 1)
    first = pltpu.make_async_copy(acc1, v1_ref, sem.at[0])
    first.start()

    @pl.loop(0, n_occ // 4)
    def _(block):
        for u in range(4):
            i = block * 4 + u
            v2[i, :head * GROUP, :] = acc2[i, n_occ:n_occ + head * GROUP, :n_vir]
            for group in range(moved):
                value = None
                for t, runs in enumerate(slots):
                    for g, src, dst, _count in runs:
                        if g == group:
                            piece = acc2[i, t * GROUP:(t + 1) * GROUP, :]
                            if (src - dst) % LANES:
                                piece = pltpu.roll(piece, (src - dst) % LANES, 1)
                            value = piece if value is None else jnp.where(lane < src, value, piece)
                v2[i, (head + group) * GROUP:(head + group + 1) * GROUP, :] = value[:, :n_vir]

    second = pltpu.make_async_copy(v2, v2_ref, sem.at[1])
    second.start()
    first.wait()
    second.wait()


def solution(mesh):
    n_dev = mesh.shape['dev']

    def local_part(ao_rows, c_occ, c_vir):
        rows, n_ao = ao_rows.shape[:2]
        n_occ, n_vir = c_occ.shape[1], c_vir.shape[1]
        assert n_occ == n_dev
        q_chunk, n_buf, pitch = 32, 3, n_ao + 8
        keep, unroll = 14, 8
        block_rows = keep * GROUP
        n_mo = n_occ + n_vir
        acc1, acc2 = pl.pallas_call(
            functools.partial(_kernel, n_dev, rows, n_ao, n_occ, n_vir, q_chunk, n_buf, pitch, keep, unroll),
            out_shape=(pltpu.VMEM((n_vir, n_occ, n_vir), F32),
                       pltpu.VMEM((n_occ, block_rows, LANES), F32)),
            in_specs=[pl.BlockSpec(memory_space=pl.ANY),
                      pl.BlockSpec(memory_space=pltpu.VMEM),
                      pl.BlockSpec(memory_space=pltpu.VMEM)],
            out_specs=(pl.BlockSpec(memory_space=pltpu.VMEM), pl.BlockSpec(memory_space=pltpu.VMEM)),
            scratch_shapes=[
                pltpu.VMEM((n_buf, q_chunk, n_ao, n_ao), BF16),
                pltpu.VMEM((n_occ * pitch, LANES), F32),
                pltpu.VMEM((n_occ * pitch, LANES), F32),
                pltpu.VMEM((2 * LANES, 2 * LANES), BF16),
                pltpu.VMEM((n_mo, n_ao), BF16),
                pltpu.VMEM((unroll, n_ao, LANES), BF16),
                pltpu.VMEM((unroll, n_ao, LANES), BF16),
                pltpu.VMEM((unroll * n_occ, n_ao), BF16),
                pltpu.VMEM((unroll * n_occ, n_ao), BF16),
                pltpu.VMEM((rows, n_dev, block_rows, LANES), BF16),
                pltpu.VMEM((rows, n_dev, block_rows, LANES), BF16),
                pltpu.VMEM((n_mo, n_dev * TILE), F32),
                pltpu.VMEM((n_mo * TILE, n_dev * TILE), BF16),
                pltpu.SemaphoreType.DMA((n_buf,)),
                pltpu.SemaphoreType.DMA((rows,)),
                pltpu.SemaphoreType.DMA((rows,)),
            ],
            compiler_params=pltpu.CompilerParams(collective_id=0, has_side_effects=True,
                                                 vmem_limit_bytes=44 * 1024 * 1024),
        )(ao_rows, c_occ.T, c_vir)
        v1, v2 = pl.pallas_call(
            functools.partial(_unpack, n_occ, n_vir, keep),
            out_shape=(jax.ShapeDtypeStruct((n_vir, n_occ, n_vir), F32),
                       jax.ShapeDtypeStruct((n_occ, n_vir, n_vir), F32)),
            in_specs=[pl.BlockSpec(memory_space=pltpu.VMEM)] * 2,
            out_specs=(pl.BlockSpec(memory_space=pl.ANY), pl.BlockSpec(memory_space=pl.ANY)),
            scratch_shapes=[pltpu.VMEM((n_occ, n_vir, n_vir), F32), pltpu.SemaphoreType.DMA((2,))],
            compiler_params=pltpu.CompilerParams(vmem_limit_bytes=8 * 1024 * 1024),
        )(acc1, acc2)
        return v1.transpose(0, 2, 1), v2

    return jax.shard_map(local_part, mesh=mesh,
                         in_specs=(P(('frag', 'dev')), P('frag'), P('frag')),
                         out_specs=(P('frag', None, 'dev'), P('frag', None, 'dev')),
                         check_vma=False)
```

```python
import functools

import jax
import jax.numpy as jnp
from jax import lax
from jax.experimental import pallas as pl
from jax.experimental.pallas import tpu as pltpu
from jax.sharding import PartitionSpec as P

F32 = jnp.float32
BF16 = jnp.bfloat16
LANES = 128
TILE = 16
GROUP = 8


def _dot(lhs, rhs):
    return lax.dot_general(lhs, rhs, (((1,), (0,)), ((), ())), preferred_element_type=F32)


def _pieces(n_vir, moved):
    spare = LANES - n_vir
    slots = []
    for t in range(-(-moved * n_vir // spare)):
        runs = []
        col, end = t * spare, min((t + 1) * spare, moved * n_vir)
        at = n_vir
        while col < end:
            count = min(end, (col // n_vir + 1) * n_vir) - col
            runs.append((col // n_vir, col % n_vir, at, count))
            col, at = col + count, at + count
        slots.append(runs)
    return slots


def _kernel(n_dev, rows, n_ao, n_occ, n_vir, q_chunk, n_buf, pitch, keep, unroll,
            a_hbm, cot_hbm, cv_hbm, acc1, acc2,
            cot_ref, cv_ref, abuf, tb0, tb1, w2, ct, hov0, hov1, hoo0, hoo1, sb, rb, rep, wk, csem, asem, ssem, rsem):
    me = lax.axis_index('dev')
    hov, hoo = (hov0, hov1), (hoo0, hoo1)
    n_chunk = n_ao // q_chunk
    n_half = n_dev // 2
    total = rows * n_chunk
    moved = (n_occ + n_vir) // GROUP - keep
    slots = _pieces(n_vir, moved)
    block_rows = keep * GROUP

    def fetch(chunk):
        slot = lax.rem(chunk, n_buf)
        return pltpu.make_async_copy(
            a_hbm.at[chunk // n_chunk, pl.ds(lax.rem(chunk, n_chunk) * q_chunk, q_chunk)],
            abuf.at[slot], asem.at[slot])

    coefs = (pltpu.make_async_copy(cot_hbm, cot_ref, csem.at[0]),
             pltpu.make_async_copy(cv_hbm, cv_ref, csem.at[1]))
    for copy in coefs:
        copy.start()
    for first in range(n_buf):
        fetch(jnp.int32(first)).start()

    barrier = pltpu.get_barrier_semaphore()

    @pl.loop(1, n_dev)
    def _(k):
        pl.semaphore_signal(barrier, inc=1, device_id={'dev': lax.rem(me + k, n_dev)},
                            device_id_type=pl.DeviceIdType.MESH)

    acc1[...] = jnp.zeros_like(acc1)
    acc2[...] = jnp.zeros_like(acc2)
    w2[...] = jnp.zeros_like(w2)
    for copy in coefs:
        copy.wait()

    w2[:n_ao, :n_vir] = cv_ref[...]
    w2[:n_ao, LANES:LANES + n_occ] = cot_ref[...].astype(F32).T.astype(BF16)
    ct[:n_occ, :] = cot_ref[...]
    ct[n_occ:, :] = cv_ref[...].astype(F32).T.astype(BF16)
    lane = lax.broadcasted_iota(jnp.int32, (GROUP, LANES), 1)

    pl.semaphore_wait(barrier, n_dev - 1)

    def send(row, step):
        return pltpu.make_async_remote_copy(
            src_ref=sb.at[row, step], dst_ref=rb.at[row, step],
            send_sem=ssem.at[row], recv_sem=rsem.at[row, step // n_half],
            device_id={'dev': lax.rem(me + 1 + step, n_dev)}, device_id_type=pl.DeviceIdType.MESH)

    @pl.loop(0, rows)
    def _(row):
        @pl.loop(0, n_chunk)
        def _(part):
            chunk = row * n_chunk + part
            slot = lax.rem(chunk, n_buf)
            fetch(chunk).wait()

            for q in range(q_chunk):
                t = _dot(cot_ref[...], abuf[slot, q])
                at = pl.ds(part * q_chunk + q, n_occ, stride=pitch)
                tb0[at, :] = t[:, :LANES]
                tb1[at, :] = jnp.pad(t[:, LANES:], ((0, 0), (0, 2 * LANES - n_ao)))

            @pl.when(chunk + n_buf < total)
            def _():
                fetch(chunk + n_buf).start()

        def owner_of(step):
            return lax.rem(me + 1 + step, n_dev)

        def half(group):
            parts = []
            for u in range(unroll):
                at = pl.ds(pl.multiple_of(owner_of(group * unroll + u) * pitch, 8), n_ao)
                parts.append(jnp.concatenate([tb0[at, :].astype(BF16), tb1[at, :].astype(BF16)], axis=1))
            h = _dot(jnp.concatenate(parts, axis=0), w2[...])
            for u in range(unroll):
                at = slice(u * n_ao, (u + 1) * n_ao)
                hov[group % 2][u] = h[at, :LANES].astype(BF16)
                hoo[group % 2][u * n_occ:(u + 1) * n_occ, :] = h[at, LANES:LANES + n_occ].T.astype(BF16)

        def full(group):
            goo = _dot(hoo[group % 2][...], w2[:n_ao, :LANES])
            for u in range(0, unroll, 2):
                pair = _dot(ct[n_occ:, :], jnp.concatenate([hov[group % 2][u], hov[group % 2][u + 1]], axis=1))
                for v in range(2):
                    gov = pair[:, v * LANES:(v + 1) * LANES]
                    first = (u + v) * n_occ
                    groups = [goo[first + g * GROUP:first + (g + 1) * GROUP] for g in range(n_occ // GROUP)]
                    groups += [gov[g * GROUP:(g + 1) * GROUP] for g in range(n_vir // GROUP)]
                    out = []
                    for t_, value in enumerate(groups[:keep]):
                        for part, src, dst, _count in (slots[t_] if t_ < len(slots) else ()):
                            tail = groups[keep + part]
                            if (dst - src) % LANES:
                                tail = pltpu.roll(tail, (dst - src) % LANES, 1)
                            value = jnp.where(lane < dst, value, tail)
                        out.append(value)
                    sb[row, group * unroll + u + v] = jnp.concatenate(out, axis=0).astype(BF16)

        n_group = n_dev // unroll
        half(0)
        for group in range(n_group):
            if group + 1 < n_group:
                half(group + 1)
            full(group)
            first, last = group * unroll, (group + 1) * unroll
            for step in range(max(first - 2, 0), last - 2):
                send(row, step).start()
        rb[row, n_dev - 1] = sb[row, n_dev - 1]
        send(row, n_dev - 2).start()

    ident = (lax.broadcasted_iota(jnp.int32, (TILE, n_dev * TILE), 1) % TILE
             == lax.broadcasted_iota(jnp.int32, (TILE, n_dev * TILE), 0))
    source = me - 1 - lax.broadcasted_iota(jnp.int32, (n_ao, n_dev * TILE), 1) // TILE
    owner = jnp.where(source < 0, source + n_dev, source) * rows
    place = lax.broadcasted_iota(jnp.int32, (n_ao, n_dev * TILE), 0)
    n_tile = block_rows // TILE
    oo_rows = n_occ * TILE

    def weights(row):
        pick = jnp.where(place == owner + row, 1.0, 0.0).astype(BF16)
        rep[...] = _dot(ct[...], pick)

        @pl.loop(0, (n_occ + n_vir) // 8)
        def _(block):
            for u in range(8):
                i = block * 8 + u
                value = jnp.where(ident, rep[pl.ds(i, 1), :], 0.0).astype(BF16)
                wk[pl.ds(pl.multiple_of(i * TILE, TILE), TILE), :] = value

    def arrived(row, part):
        blocks = rb.at[row, pl.ds(part * n_half, n_half - part)]
        pltpu.make_async_copy(blocks, blocks, rsem.at[row, part]).wait()

    def contract(row, low, high):
        cols = slice(low * TILE, high * TILE)

        def tiles(first, count):
            parts = [rb[row, low:high, t * TILE:(t + 1) * TILE, :].reshape((high - low) * TILE, LANES)
                     for t in range(first, first + count)]
            return parts[0] if count == 1 else jnp.concatenate(parts, axis=1)

        for first in range(0, n_tile, 2):
            count = min(2, n_tile - first)
            out = _dot(wk[:oo_rows, cols], tiles(first, count))
            for c in range(count):
                at = slice((first + c) * TILE, (first + c + 1) * TILE)
                acc2[:, at, :] += out[:, c * LANES:(c + 1) * LANES].reshape(n_occ, TILE, LANES)

        n_block = 4
        span = n_vir // n_block
        rhs = tiles(0, n_occ // TILE)

        @pl.loop(0, n_block)
        def _(block):
            at = pl.ds(pl.multiple_of(oo_rows + block * (span * TILE), TILE), span * TILE)
            out = _dot(wk[at, cols], rhs)
            for c in range(n_occ // TILE):
                acc1[pl.ds(block * span, span), c * TILE:(c + 1) * TILE, :] += (
                    out[:, c * LANES:c * LANES + n_vir].reshape(span, TILE, n_vir))

    @pl.loop(0, rows - 1)
    def _(row):
        weights(row)
        arrived(row, 0)
        arrived(row, 1)
        contract(row, 0, n_dev)

    weights(rows - 1)
    for part in range(2):
        arrived(rows - 1, part)
        contract(rows - 1, part * n_half, (part + 1) * n_half)

    for row in range(rows):
        pltpu.make_async_copy(sb.at[row, pl.ds(0, n_dev - 1)], sb.at[row, pl.ds(0, n_dev - 1)],
                              ssem.at[row]).wait()


def _unpack(n_occ, n_vir, keep, acc1, acc2, v1_ref, v2_ref, v2, sem):
    moved = (n_occ + n_vir) // GROUP - keep
    head = n_vir // GROUP - moved
    slots = _pieces(n_vir, moved)
    lane = lax.broadcasted_iota(jnp.int32, (GROUP, LANES), 1)
    copies = [pltpu.make_async_copy(acc1, v1_ref, sem.at[0])]
    copies[0].start()
    for i in range(n_occ):
        v2[i, :head * GROUP, :] = acc2[i, n_occ:n_occ + head * GROUP, :n_vir]
        for group in range(moved):
            value = None
            for t, runs in enumerate(slots):
                for g, src, dst, _count in runs:
                    if g == group:
                        piece = acc2[i, t * GROUP:(t + 1) * GROUP, :]
                        if (src - dst) % LANES:
                            piece = pltpu.roll(piece, (src - dst) % LANES, 1)
                        value = piece if value is None else jnp.where(lane < src, value, piece)
            v2[i, (head + group) * GROUP:(head + group + 1) * GROUP, :] = value[:, :n_vir]
        if i % 8 == 7:
            at = pl.ds(i - 7, 8)
            copies.append(pltpu.make_async_copy(v2.at[at], v2_ref.at[at], sem.at[1 + i // 8]))
            copies[-1].start()
    for copy in copies:
        copy.wait()


def solution(mesh):
    n_dev = mesh.shape['dev']

    def local_part(ao_rows, c_occ, c_vir):
        rows, n_ao = ao_rows.shape[:2]
        n_occ, n_vir = c_occ.shape[1], c_vir.shape[1]
        assert n_occ == n_dev
        q_chunk, n_buf, pitch = 32, 5, n_ao + 8
        keep, unroll = 14, 8
        block_rows = keep * GROUP
        n_mo = n_occ + n_vir
        acc1, acc2 = pl.pallas_call(
            functools.partial(_kernel, n_dev, rows, n_ao, n_occ, n_vir, q_chunk, n_buf, pitch, keep, unroll),
            out_shape=(pltpu.VMEM((n_vir, n_occ, n_vir), F32),
                       pltpu.VMEM((n_occ, block_rows, LANES), F32)),
            in_specs=[pl.BlockSpec(memory_space=pltpu.HBM)] * 3,
            out_specs=(pl.BlockSpec(memory_space=pltpu.VMEM), pl.BlockSpec(memory_space=pltpu.VMEM)),
            scratch_shapes=[
                pltpu.VMEM((n_occ, n_ao), BF16),
                pltpu.VMEM((n_ao, n_vir), BF16),
                pltpu.VMEM((n_buf, q_chunk, n_ao, n_ao), BF16),
                pltpu.VMEM((n_occ * pitch, LANES), F32),
                pltpu.VMEM((n_occ * pitch, LANES), F32),
                pltpu.VMEM((2 * LANES, 2 * LANES), BF16),
                pltpu.VMEM((n_mo, n_ao), BF16),
                pltpu.VMEM((unroll, n_ao, LANES), BF16),
                pltpu.VMEM((unroll, n_ao, LANES), BF16),
                pltpu.VMEM((unroll * n_occ, n_ao), BF16),
                pltpu.VMEM((unroll * n_occ, n_ao), BF16),
                pltpu.VMEM((rows, n_dev, block_rows, LANES), BF16),
                pltpu.VMEM((rows, n_dev, block_rows, LANES), BF16),
                pltpu.VMEM((n_mo, n_dev * TILE), F32),
                pltpu.VMEM((n_mo * TILE, n_dev * TILE), BF16),
                pltpu.SemaphoreType.DMA((2,)),
                pltpu.SemaphoreType.DMA((n_buf,)),
                pltpu.SemaphoreType.DMA((rows,)),
                pltpu.SemaphoreType.DMA((rows, 2)),
            ],
            compiler_params=pltpu.CompilerParams(collective_id=0, has_side_effects=True,
                                                 vmem_limit_bytes=44 * 1024 * 1024),
        )(ao_rows, *(pltpu.with_memory_space_constraint(c, pltpu.HBM) for c in (c_occ.T, c_vir)))
        v1, v2 = pl.pallas_call(
            functools.partial(_unpack, n_occ, n_vir, keep),
            out_shape=(jax.ShapeDtypeStruct((n_vir, n_occ, n_vir), F32),
                       jax.ShapeDtypeStruct((n_occ, n_vir, n_vir), F32)),
            in_specs=[pl.BlockSpec(memory_space=pltpu.VMEM)] * 2,
            out_specs=(pl.BlockSpec(memory_space=pl.ANY), pl.BlockSpec(memory_space=pl.ANY)),
            scratch_shapes=[pltpu.VMEM((n_occ, n_vir, n_vir), F32), pltpu.SemaphoreType.DMA((1 + n_occ // 8,))],
            compiler_params=pltpu.CompilerParams(vmem_limit_bytes=8 * 1024 * 1024),
        )(acc1, acc2)
        return v1.transpose(0, 2, 1), v2

    return jax.shard_map(local_part, mesh=mesh,
                         in_specs=(P(('frag', 'dev')), P('frag'), P('frag')),
                         out_specs=(P('frag', None, 'dev'), P('frag', None, 'dev')),
                         check_vma=False)
```

```python
import functools
import math

import jax
import jax.numpy as jnp
from jax import lax
from jax.experimental import pallas as pl
from jax.experimental.pallas import tpu as pltpu
from jax.sharding import PartitionSpec as P

F32 = jnp.float32
BF16 = jnp.bfloat16
LANES = 128
TILE = 16
GROUP = 8


def _dot(lhs, rhs):
    return lax.dot_general(lhs, rhs, (((1,), (0,)), ((), ())), preferred_element_type=F32)


def _pieces(n_vir, moved):
    spare = LANES - n_vir
    slots = []
    for t in range(-(-moved * n_vir // spare)):
        runs = []
        col, end = t * spare, min((t + 1) * spare, moved * n_vir)
        at = n_vir
        while col < end:
            count = min(end, (col // n_vir + 1) * n_vir) - col
            runs.append((col // n_vir, col % n_vir, at, count))
            col, at = col + count, at + count
        slots.append(runs)
    return slots


def _order(side):
    def hops(d):
        return min(d, side - d)

    left = {(dx, dy) for dx in range(side) for dy in range(side)}
    chips = []
    for dx, dy in sorted(left, key=lambda c: (-(hops(c[0]) > 0) - (hops(c[1]) > 0),
                                              abs(hops(c[0]) - hops(c[1])), hops(c[0]), c)):
        for chip in ((dx, dy), (-dx % side, -dy % side), (dy, -dx % side), (-dy % side, dx)):
            if chip in left:
                left.remove(chip)
                chips.append(chip)
    return [(dx, dy, other) for dx, dy in chips for other in (1, 0)]


def _kernel(n_dev, rows, n_ao, n_occ, n_vir, q_chunk, n_buf, pitch, keep, unroll,
            a_hbm, cot_hbm, cv_hbm, acc1, acc2,
            cot_ref, cv_ref, abuf, tb0, tb1, w2, ct, hov0, hov1, hoo0, hoo1, sb, rb, rep, wk, csem, asem, ssem, rsem):
    me = lax.axis_index('dev')
    hov, hoo = (hov0, hov1), (hoo0, hoo1)
    side = math.isqrt(n_dev // 2)
    core, cx, cy = lax.rem(me, 2), lax.rem(me // 2, side), me // (2 * side)
    order = _order(side)

    def partner(step, away):
        dx, dy, other = order[step]
        there = lax.rem(core + other, 2)
        sign = away * (1 - 2 * (core if away > 0 else there))
        return ((lax.rem(cy + dy * sign + side, side) * side + lax.rem(cx + dx * sign + side, side)) * 2
                + there)

    n_chunk = n_ao // q_chunk
    n_half = n_dev // 2
    total = rows * n_chunk
    moved = (n_occ + n_vir) // GROUP - keep
    slots = _pieces(n_vir, moved)
    block_rows = keep * GROUP

    def fetch(chunk):
        slot = lax.rem(chunk, n_buf)
        return pltpu.make_async_copy(
            a_hbm.at[chunk // n_chunk, pl.ds(lax.rem(chunk, n_chunk) * q_chunk, q_chunk)],
            abuf.at[slot], asem.at[slot])

    coefs = (pltpu.make_async_copy(cot_hbm, cot_ref, csem.at[0]),
             pltpu.make_async_copy(cv_hbm, cv_ref, csem.at[1]))
    for copy in coefs:
        copy.start()
    for first in range(n_buf):
        fetch(jnp.int32(first)).start()

    barrier = pltpu.get_barrier_semaphore()

    @pl.loop(1, n_dev)
    def _(k):
        pl.semaphore_signal(barrier, inc=1, device_id={'dev': lax.rem(me + k, n_dev)},
                            device_id_type=pl.DeviceIdType.MESH)

    acc1[...] = jnp.zeros_like(acc1)
    acc2[...] = jnp.zeros_like(acc2)
    w2[...] = jnp.zeros_like(w2)
    for copy in coefs:
        copy.wait()

    w2[:n_ao, :n_vir] = cv_ref[...]
    w2[:n_ao, LANES:LANES + n_occ] = cot_ref[...].astype(F32).T.astype(BF16)
    ct[:n_occ, :] = cot_ref[...]
    ct[n_occ:, :] = cv_ref[...].astype(F32).T.astype(BF16)
    lane = lax.broadcasted_iota(jnp.int32, (GROUP, LANES), 1)

    pl.semaphore_wait(barrier, n_dev - 1)

    def send(row, step):
        return pltpu.make_async_remote_copy(
            src_ref=sb.at[row, step], dst_ref=rb.at[row, step],
            send_sem=ssem.at[row], recv_sem=rsem.at[row, step // n_half],
            device_id={'dev': partner(step, 1)}, device_id_type=pl.DeviceIdType.MESH)

    @pl.loop(0, rows)
    def _(row):
        @pl.loop(0, n_chunk)
        def _(part):
            chunk = row * n_chunk + part
            slot = lax.rem(chunk, n_buf)
            fetch(chunk).wait()

            for q in range(q_chunk):
                t = _dot(cot_ref[...], abuf[slot, q])
                at = pl.ds(part * q_chunk + q, n_occ, stride=pitch)
                tb0[at, :] = t[:, :LANES]
                tb1[at, :] = jnp.pad(t[:, LANES:], ((0, 0), (0, 2 * LANES - n_ao)))

            @pl.when(chunk + n_buf < total)
            def _():
                fetch(chunk + n_buf).start()

        def half(group):
            parts = []
            for u in range(unroll):
                at = pl.ds(pl.multiple_of(partner(group * unroll + u, 1) * pitch, 8), n_ao)
                parts.append(jnp.concatenate([tb0[at, :].astype(BF16), tb1[at, :].astype(BF16)], axis=1))
            h = _dot(jnp.concatenate(parts, axis=0), w2[...])
            for u in range(unroll):
                at = slice(u * n_ao, (u + 1) * n_ao)
                hov[group % 2][u] = h[at, :LANES].astype(BF16)
                hoo[group % 2][u * n_occ:(u + 1) * n_occ, :] = h[at, LANES:LANES + n_occ].T.astype(BF16)

        def full(group):
            goo = _dot(hoo[group % 2][...], w2[:n_ao, :LANES])
            for u in range(0, unroll, 2):
                pair = _dot(ct[n_occ:, :], jnp.concatenate([hov[group % 2][u], hov[group % 2][u + 1]], axis=1))
                for v in range(2):
                    gov = pair[:, v * LANES:(v + 1) * LANES]
                    first = (u + v) * n_occ
                    groups = [goo[first + g * GROUP:first + (g + 1) * GROUP] for g in range(n_occ // GROUP)]
                    groups += [gov[g * GROUP:(g + 1) * GROUP] for g in range(n_vir // GROUP)]
                    out = []
                    for t_, value in enumerate(groups[:keep]):
                        for part, src, dst, _count in (slots[t_] if t_ < len(slots) else ()):
                            tail = groups[keep + part]
                            if (dst - src) % LANES:
                                tail = pltpu.roll(tail, (dst - src) % LANES, 1)
                            value = jnp.where(lane < dst, value, tail)
                        out.append(value)
                    sb[row, group * unroll + u + v] = jnp.concatenate(out, axis=0).astype(BF16)

        n_group = n_dev // unroll
        half(0)
        for group in range(n_group):
            if group + 1 < n_group:
                half(group + 1)
            full(group)
            first, last = group * unroll, (group + 1) * unroll
            for step in range(max(first - 2, 0), last - 2):
                send(row, step).start()
        rb[row, n_dev - 1] = sb[row, n_dev - 1]
        send(row, n_dev - 2).start()

    ident = (lax.broadcasted_iota(jnp.int32, (TILE, n_dev * TILE), 1) % TILE
             == lax.broadcasted_iota(jnp.int32, (TILE, n_dev * TILE), 0))
    slot = lax.broadcasted_iota(jnp.int32, (1, n_dev * TILE), 1) // TILE
    owner = jnp.zeros_like(slot)
    for step in range(n_dev):
        owner = jnp.where(slot == step, partner(step, -1) * rows, owner)
    place = lax.broadcasted_iota(jnp.int32, (n_ao, n_dev * TILE), 0)
    n_tile = block_rows // TILE
    oo_rows = n_occ * TILE

    def weights(row):
        pick = jnp.where(place == owner + row, 1.0, 0.0).astype(BF16)
        rep[...] = _dot(ct[...], pick)

        @pl.loop(0, (n_occ + n_vir) // 8)
        def _(block):
            for u in range(8):
                i = block * 8 + u
                value = jnp.where(ident, rep[pl.ds(i, 1), :], 0.0).astype(BF16)
                wk[pl.ds(pl.multiple_of(i * TILE, TILE), TILE), :] = value

    def arrived(row, part):
        blocks = rb.at[row, pl.ds(part * n_half, n_half - part)]
        pltpu.make_async_copy(blocks, blocks, rsem.at[row, part]).wait()

    def contract(row, low, high):
        cols = slice(low * TILE, high * TILE)

        def tiles(first, count):
            parts = [rb[row, low:high, t * TILE:(t + 1) * TILE, :].reshape((high - low) * TILE, LANES)
                     for t in range(first, first + count)]
            return parts[0] if count == 1 else jnp.concatenate(parts, axis=1)

        for first in range(0, n_tile, 2):
            count = min(2, n_tile - first)
            out = _dot(wk[:oo_rows, cols], tiles(first, count))
            for c in range(count):
                at = slice((first + c) * TILE, (first + c + 1) * TILE)
                acc2[:, at, :] += out[:, c * LANES:(c + 1) * LANES].reshape(n_occ, TILE, LANES)

        n_block = 4
        span = n_vir // n_block
        rhs = tiles(0, n_occ // TILE)

        @pl.loop(0, n_block)
        def _(block):
            at = pl.ds(pl.multiple_of(oo_rows + block * (span * TILE), TILE), span * TILE)
            out = _dot(wk[at, cols], rhs)
            for c in range(n_occ // TILE):
                acc1[pl.ds(block * span, span), c * TILE:(c + 1) * TILE, :] += (
                    out[:, c * LANES:c * LANES + n_vir].reshape(span, TILE, n_vir))

    @pl.loop(0, rows - 1)
    def _(row):
        weights(row)
        arrived(row, 0)
        arrived(row, 1)
        contract(row, 0, n_dev)

    weights(rows - 1)
    for part in range(2):
        arrived(rows - 1, part)
        contract(rows - 1, part * n_half, (part + 1) * n_half)

    for row in range(rows):
        pltpu.make_async_copy(sb.at[row, pl.ds(0, n_dev - 1)], sb.at[row, pl.ds(0, n_dev - 1)],
                              ssem.at[row]).wait()


def _unpack(n_occ, n_vir, keep, acc1, acc2, v1_ref, v2_ref, v2, sem):
    moved = (n_occ + n_vir) // GROUP - keep
    head = n_vir // GROUP - moved
    slots = _pieces(n_vir, moved)
    lane = lax.broadcasted_iota(jnp.int32, (GROUP, LANES), 1)
    copies = [pltpu.make_async_copy(acc1, v1_ref, sem.at[0])]
    copies[0].start()
    for i in range(n_occ):
        v2[i, :head * GROUP, :] = acc2[i, n_occ:n_occ + head * GROUP, :n_vir]
        for group in range(moved):
            value = None
            for t, runs in enumerate(slots):
                for g, src, dst, _count in runs:
                    if g == group:
                        piece = acc2[i, t * GROUP:(t + 1) * GROUP, :]
                        if (src - dst) % LANES:
                            piece = pltpu.roll(piece, (src - dst) % LANES, 1)
                        value = piece if value is None else jnp.where(lane < src, value, piece)
            v2[i, (head + group) * GROUP:(head + group + 1) * GROUP, :] = value[:, :n_vir]
        if i % 8 == 7:
            at = pl.ds(i - 7, 8)
            copies.append(pltpu.make_async_copy(v2.at[at], v2_ref.at[at], sem.at[1 + i // 8]))
            copies[-1].start()
    for copy in copies:
        copy.wait()


def solution(mesh):
    n_dev = mesh.shape['dev']

    def local_part(ao_rows, c_occ, c_vir):
        rows, n_ao = ao_rows.shape[:2]
        n_occ, n_vir = c_occ.shape[1], c_vir.shape[1]
        assert n_occ == n_dev
        q_chunk, n_buf, pitch = 32, 5, n_ao + 8
        keep, unroll = 14, 8
        block_rows = keep * GROUP
        n_mo = n_occ + n_vir
        acc1, acc2 = pl.pallas_call(
            functools.partial(_kernel, n_dev, rows, n_ao, n_occ, n_vir, q_chunk, n_buf, pitch, keep, unroll),
            out_shape=(pltpu.VMEM((n_vir, n_occ, n_vir), F32),
                       pltpu.VMEM((n_occ, block_rows, LANES), F32)),
            in_specs=[pl.BlockSpec(memory_space=pltpu.HBM)] * 3,
            out_specs=(pl.BlockSpec(memory_space=pltpu.VMEM), pl.BlockSpec(memory_space=pltpu.VMEM)),
            scratch_shapes=[
                pltpu.VMEM((n_occ, n_ao), BF16),
                pltpu.VMEM((n_ao, n_vir), BF16),
                pltpu.VMEM((n_buf, q_chunk, n_ao, n_ao), BF16),
                pltpu.VMEM((n_occ * pitch, LANES), F32),
                pltpu.VMEM((n_occ * pitch, LANES), F32),
                pltpu.VMEM((2 * LANES, 2 * LANES), BF16),
                pltpu.VMEM((n_mo, n_ao), BF16),
                pltpu.VMEM((unroll, n_ao, LANES), BF16),
                pltpu.VMEM((unroll, n_ao, LANES), BF16),
                pltpu.VMEM((unroll * n_occ, n_ao), BF16),
                pltpu.VMEM((unroll * n_occ, n_ao), BF16),
                pltpu.VMEM((rows, n_dev, block_rows, LANES), BF16),
                pltpu.VMEM((rows, n_dev, block_rows, LANES), BF16),
                pltpu.VMEM((n_mo, n_dev * TILE), F32),
                pltpu.VMEM((n_mo * TILE, n_dev * TILE), BF16),
                pltpu.SemaphoreType.DMA((2,)),
                pltpu.SemaphoreType.DMA((n_buf,)),
                pltpu.SemaphoreType.DMA((rows,)),
                pltpu.SemaphoreType.DMA((rows, 2)),
            ],
            compiler_params=pltpu.CompilerParams(collective_id=0, has_side_effects=True,
                                                 vmem_limit_bytes=44 * 1024 * 1024),
        )(ao_rows, *(pltpu.with_memory_space_constraint(c, pltpu.HBM) for c in (c_occ.T, c_vir)))
        v1, v2 = pl.pallas_call(
            functools.partial(_unpack, n_occ, n_vir, keep),
            out_shape=(jax.ShapeDtypeStruct((n_vir, n_occ, n_vir), F32),
                       jax.ShapeDtypeStruct((n_occ, n_vir, n_vir), F32)),
            in_specs=[pl.BlockSpec(memory_space=pltpu.VMEM)] * 2,
            out_specs=(pl.BlockSpec(memory_space=pl.ANY), pl.BlockSpec(memory_space=pl.ANY)),
            scratch_shapes=[pltpu.VMEM((n_occ, n_vir, n_vir), F32), pltpu.SemaphoreType.DMA((1 + n_occ // 8,))],
            compiler_params=pltpu.CompilerParams(vmem_limit_bytes=8 * 1024 * 1024),
        )(acc1, acc2)
        return v1.transpose(0, 2, 1), v2

    return jax.shard_map(local_part, mesh=mesh,
                         in_specs=(P(('frag', 'dev')), P('frag'), P('frag')),
                         out_specs=(P('frag', None, 'dev'), P('frag', None, 'dev')),
                         check_vma=False)
```

```python
import functools
import math

import jax
import jax.numpy as jnp
from jax import lax
from jax.experimental import pallas as pl
from jax.experimental.pallas import tpu as pltpu
from jax.sharding import PartitionSpec as P

F32 = jnp.float32
BF16 = jnp.bfloat16
LANES = 128
TILE = 16
GROUP = 8


def _dot(lhs, rhs):
    return lax.dot_general(lhs, rhs, (((1,), (0,)), ((), ())), preferred_element_type=F32)


def _pieces(n_vir, moved):
    spare = LANES - n_vir
    slots = []
    for t in range(-(-moved * n_vir // spare)):
        runs = []
        col, end = t * spare, min((t + 1) * spare, moved * n_vir)
        at = n_vir
        while col < end:
            count = min(end, (col // n_vir + 1) * n_vir) - col
            runs.append((col // n_vir, col % n_vir, at, count))
            col, at = col + count, at + count
        slots.append(runs)
    return slots


def _order(side):
    def hops(d):
        return min(d, side - d)

    left = {(dx, dy) for dx in range(side) for dy in range(side)}
    chips = []
    for dx, dy in sorted(left, key=lambda c: (-(hops(c[0]) > 0) - (hops(c[1]) > 0),
                                              abs(hops(c[0]) - hops(c[1])), hops(c[0]), c)):
        for chip in ((dx, dy), (-dx % side, -dy % side), (dy, -dx % side), (-dy % side, dx)):
            if chip in left:
                left.remove(chip)
                chips.append(chip)
    return [(dx, dy, other) for dx, dy in chips for other in (1, 0)]


def _kernel(n_dev, rows, n_ao, n_occ, n_vir, q_chunk, n_buf, pitch, keep, unroll,
            a_hbm, cot_hbm, cv_hbm, acc1, acc2,
            cot_ref, cv_ref, abuf, tb0, tb1, w2, ct, hov0, hov1, hoo0, hoo1, sb, rb, rep, wk, csem, asem, ssem, rsem):
    me = lax.axis_index('dev')
    hov, hoo = (hov0, hov1), (hoo0, hoo1)
    side = math.isqrt(n_dev // 2)
    core, cx, cy = lax.rem(me, 2), lax.rem(me // 2, side), me // (2 * side)
    order = _order(side)

    def partner(step, away):
        dx, dy, other = order[step]
        there = lax.rem(core + other, 2)
        sign = away * (1 - 2 * (core if away > 0 else there))
        return ((lax.rem(cy + dy * sign + side, side) * side + lax.rem(cx + dx * sign + side, side)) * 2
                + there)

    n_chunk = n_ao // q_chunk
    n_half = n_dev // 2
    total = rows * n_chunk
    moved = (n_occ + n_vir) // GROUP - keep
    slots = _pieces(n_vir, moved)
    block_rows = keep * GROUP
    cuts = (0, 4 * TILE, block_rows)

    def fetch(chunk):
        slot = lax.rem(chunk, n_buf)
        return pltpu.make_async_copy(
            a_hbm.at[chunk // n_chunk, pl.ds(lax.rem(chunk, n_chunk) * q_chunk, q_chunk)],
            abuf.at[slot], asem.at[slot])

    coefs = (pltpu.make_async_copy(cot_hbm, cot_ref, csem.at[0]),
             pltpu.make_async_copy(cv_hbm, cv_ref, csem.at[1]))
    for copy in coefs:
        copy.start()
    for first in range(n_buf):
        fetch(jnp.int32(first)).start()

    barrier = pltpu.get_barrier_semaphore()

    @pl.loop(1, n_dev)
    def _(k):
        pl.semaphore_signal(barrier, inc=1, device_id={'dev': lax.rem(me + k, n_dev)},
                            device_id_type=pl.DeviceIdType.MESH)

    acc1[...] = jnp.zeros_like(acc1)
    acc2[...] = jnp.zeros_like(acc2)
    w2[...] = jnp.zeros_like(w2)
    for copy in coefs:
        copy.wait()

    w2[:n_ao, :n_vir] = cv_ref[...]
    w2[:n_ao, LANES:LANES + n_occ] = cot_ref[...].astype(F32).T.astype(BF16)
    ct[:n_occ, :] = cot_ref[...]
    ct[n_occ:, :] = cv_ref[...].astype(F32).T.astype(BF16)
    lane = lax.broadcasted_iota(jnp.int32, (GROUP, LANES), 1)

    pl.semaphore_wait(barrier, n_dev - 1)

    def send(row, steps):
        for low, high in zip(cuts, cuts[1:]):
            for step in steps:
                pltpu.make_async_remote_copy(
                    src_ref=sb.at[row, step, low:high], dst_ref=rb.at[row, step, low:high],
                    send_sem=ssem.at[row], recv_sem=rsem.at[row, step // n_half],
                    device_id={'dev': partner(step, 1)}, device_id_type=pl.DeviceIdType.MESH).start()

    @pl.loop(0, rows)
    def _(row):
        @pl.loop(0, n_chunk)
        def _(part):
            chunk = row * n_chunk + part
            slot = lax.rem(chunk, n_buf)
            fetch(chunk).wait()

            for q in range(q_chunk):
                t = _dot(cot_ref[...], abuf[slot, q])
                at = pl.ds(part * q_chunk + q, n_occ, stride=pitch)
                tb0[at, :] = t[:, :LANES]
                tb1[at, :] = jnp.pad(t[:, LANES:], ((0, 0), (0, 2 * LANES - n_ao)))

            @pl.when(chunk + n_buf < total)
            def _():
                fetch(chunk + n_buf).start()

        def half(group):
            parts = []
            for u in range(unroll):
                at = pl.ds(pl.multiple_of(partner(group * unroll + u, 1) * pitch, 8), n_ao)
                parts.append(jnp.concatenate([tb0[at, :].astype(BF16), tb1[at, :].astype(BF16)], axis=1))
            h = _dot(jnp.concatenate(parts, axis=0), w2[...])
            for u in range(unroll):
                at = slice(u * n_ao, (u + 1) * n_ao)
                hov[group % 2][u] = h[at, :LANES].astype(BF16)
                hoo[group % 2][u * n_occ:(u + 1) * n_occ, :] = h[at, LANES:LANES + n_occ].T.astype(BF16)

        def full(group):
            goo = _dot(hoo[group % 2][...], w2[:n_ao, :LANES])
            for u in range(0, unroll, 2):
                pair = _dot(ct[n_occ:, :], jnp.concatenate([hov[group % 2][u], hov[group % 2][u + 1]], axis=1))
                for v in range(2):
                    gov = pair[:, v * LANES:(v + 1) * LANES]
                    first = (u + v) * n_occ
                    groups = [goo[first + g * GROUP:first + (g + 1) * GROUP] for g in range(n_occ // GROUP)]
                    groups += [gov[g * GROUP:(g + 1) * GROUP] for g in range(n_vir // GROUP)]
                    out = []
                    for t_, value in enumerate(groups[:keep]):
                        for part, src, dst, _count in (slots[t_] if t_ < len(slots) else ()):
                            tail = groups[keep + part]
                            if (dst - src) % LANES:
                                tail = pltpu.roll(tail, (dst - src) % LANES, 1)
                            value = jnp.where(lane < dst, value, tail)
                        out.append(value)
                    sb[row, group * unroll + u + v] = jnp.concatenate(out, axis=0).astype(BF16)

        n_group = n_dev // unroll
        half(0)
        for group in range(n_group):
            if group + 1 < n_group:
                half(group + 1)
            full(group)
            first, last = group * unroll, (group + 1) * unroll
            send(row, range(max(first - 2, 0), last - 2))
        rb[row, n_dev - 1] = sb[row, n_dev - 1]
        send(row, [n_dev - 2])

    ident = (lax.broadcasted_iota(jnp.int32, (TILE, n_dev * TILE), 1) % TILE
             == lax.broadcasted_iota(jnp.int32, (TILE, n_dev * TILE), 0))
    slot = lax.broadcasted_iota(jnp.int32, (1, n_dev * TILE), 1) // TILE
    owner = jnp.zeros_like(slot)
    for step in range(n_dev):
        owner = jnp.where(slot == step, partner(step, -1) * rows, owner)
    place = lax.broadcasted_iota(jnp.int32, (n_ao, n_dev * TILE), 0)
    n_tile = block_rows // TILE
    oo_rows = n_occ * TILE

    def weights(row):
        pick = jnp.where(place == owner + row, 1.0, 0.0).astype(BF16)
        rep[...] = _dot(ct[...], pick)

        @pl.loop(0, (n_occ + n_vir) // 8)
        def _(block):
            for u in range(8):
                i = block * 8 + u
                value = jnp.where(ident, rep[pl.ds(i, 1), :], 0.0).astype(BF16)
                wk[pl.ds(pl.multiple_of(i * TILE, TILE), TILE), :] = value

    def arrived(row, part):
        blocks = rb.at[row, pl.ds(part * n_half, n_half - part)]
        pltpu.make_async_copy(blocks, blocks, rsem.at[row, part]).wait()

    def contract(row, low, high):
        cols = slice(low * TILE, high * TILE)

        def tiles(first, count):
            parts = [rb[row, low:high, t * TILE:(t + 1) * TILE, :].reshape((high - low) * TILE, LANES)
                     for t in range(first, first + count)]
            return parts[0] if count == 1 else jnp.concatenate(parts, axis=1)

        for first in range(0, n_tile, 2):
            count = min(2, n_tile - first)
            out = _dot(wk[:oo_rows, cols], tiles(first, count))
            for c in range(count):
                at = slice((first + c) * TILE, (first + c + 1) * TILE)
                acc2[:, at, :] += out[:, c * LANES:(c + 1) * LANES].reshape(n_occ, TILE, LANES)

        n_block = 4
        span = n_vir // n_block
        rhs = tiles(0, n_occ // TILE)

        @pl.loop(0, n_block)
        def _(block):
            at = pl.ds(pl.multiple_of(oo_rows + block * (span * TILE), TILE), span * TILE)
            out = _dot(wk[at, cols], rhs)
            for c in range(n_occ // TILE):
                acc1[pl.ds(block * span, span), c * TILE:(c + 1) * TILE, :] += (
                    out[:, c * LANES:c * LANES + n_vir].reshape(span, TILE, n_vir))

    @pl.loop(0, rows - 1)
    def _(row):
        weights(row)
        arrived(row, 0)
        arrived(row, 1)
        contract(row, 0, n_dev)

    weights(rows - 1)
    for part in range(2):
        arrived(rows - 1, part)
        contract(rows - 1, part * n_half, (part + 1) * n_half)

    for row in range(rows):
        pltpu.make_async_copy(sb.at[row, pl.ds(0, n_dev - 1)], sb.at[row, pl.ds(0, n_dev - 1)],
                              ssem.at[row]).wait()


def _unpack(n_occ, n_vir, keep, acc1, acc2, v1_ref, v2_ref, v2, sem):
    moved = (n_occ + n_vir) // GROUP - keep
    head = n_vir // GROUP - moved
    slots = _pieces(n_vir, moved)
    lane = lax.broadcasted_iota(jnp.int32, (GROUP, LANES), 1)
    copies = [pltpu.make_async_copy(acc1, v1_ref, sem.at[0])]
    copies[0].start()
    for i in range(n_occ):
        v2[i, :head * GROUP, :] = acc2[i, n_occ:n_occ + head * GROUP, :n_vir]
        for group in range(moved):
            value = None
            for t, runs in enumerate(slots):
                for g, src, dst, _count in runs:
                    if g == group:
                        piece = acc2[i, t * GROUP:(t + 1) * GROUP, :]
                        if (src - dst) % LANES:
                            piece = pltpu.roll(piece, (src - dst) % LANES, 1)
                        value = piece if value is None else jnp.where(lane < src, value, piece)
            v2[i, (head + group) * GROUP:(head + group + 1) * GROUP, :] = value[:, :n_vir]
        if i % 8 == 7:
            at = pl.ds(i - 7, 8)
            copies.append(pltpu.make_async_copy(v2.at[at], v2_ref.at[at], sem.at[1 + i // 8]))
            copies[-1].start()
    for copy in copies:
        copy.wait()


def solution(mesh):
    n_dev = mesh.shape['dev']

    def local_part(ao_rows, c_occ, c_vir):
        rows, n_ao = ao_rows.shape[:2]
        n_occ, n_vir = c_occ.shape[1], c_vir.shape[1]
        assert n_occ == n_dev
        q_chunk, n_buf, pitch = 32, 5, n_ao + 8
        keep, unroll = 14, 8
        block_rows = keep * GROUP
        n_mo = n_occ + n_vir
        acc1, acc2 = pl.pallas_call(
            functools.partial(_kernel, n_dev, rows, n_ao, n_occ, n_vir, q_chunk, n_buf, pitch, keep, unroll),
            out_shape=(pltpu.VMEM((n_vir, n_occ, n_vir), F32),
                       pltpu.VMEM((n_occ, block_rows, LANES), F32)),
            in_specs=[pl.BlockSpec(memory_space=pltpu.HBM)] * 3,
            out_specs=(pl.BlockSpec(memory_space=pltpu.VMEM), pl.BlockSpec(memory_space=pltpu.VMEM)),
            scratch_shapes=[
                pltpu.VMEM((n_occ, n_ao), BF16),
                pltpu.VMEM((n_ao, n_vir), BF16),
                pltpu.VMEM((n_buf, q_chunk, n_ao, n_ao), BF16),
                pltpu.VMEM((n_occ * pitch, LANES), F32),
                pltpu.VMEM((n_occ * pitch, LANES), F32),
                pltpu.VMEM((2 * LANES, 2 * LANES), BF16),
                pltpu.VMEM((n_mo, n_ao), BF16),
                pltpu.VMEM((unroll, n_ao, LANES), BF16),
                pltpu.VMEM((unroll, n_ao, LANES), BF16),
                pltpu.VMEM((unroll * n_occ, n_ao), BF16),
                pltpu.VMEM((unroll * n_occ, n_ao), BF16),
                pltpu.VMEM((rows, n_dev, block_rows, LANES), BF16),
                pltpu.VMEM((rows, n_dev, block_rows, LANES), BF16),
                pltpu.VMEM((n_mo, n_dev * TILE), F32),
                pltpu.VMEM((n_mo * TILE, n_dev * TILE), BF16),
                pltpu.SemaphoreType.DMA((2,)),
                pltpu.SemaphoreType.DMA((n_buf,)),
                pltpu.SemaphoreType.DMA((rows,)),
                pltpu.SemaphoreType.DMA((rows, 2)),
            ],
            compiler_params=pltpu.CompilerParams(collective_id=0, has_side_effects=True,
                                                 vmem_limit_bytes=44 * 1024 * 1024),
        )(ao_rows, *(pltpu.with_memory_space_constraint(c, pltpu.HBM) for c in (c_occ.T, c_vir)))
        v1, v2 = pl.pallas_call(
            functools.partial(_unpack, n_occ, n_vir, keep),
            out_shape=(jax.ShapeDtypeStruct((n_vir, n_occ, n_vir), F32),
                       jax.ShapeDtypeStruct((n_occ, n_vir, n_vir), F32)),
            in_specs=[pl.BlockSpec(memory_space=pltpu.VMEM)] * 2,
            out_specs=(pl.BlockSpec(memory_space=pl.ANY), pl.BlockSpec(memory_space=pl.ANY)),
            scratch_shapes=[pltpu.VMEM((n_occ, n_vir, n_vir), F32), pltpu.SemaphoreType.DMA((1 + n_occ // 8,))],
            compiler_params=pltpu.CompilerParams(vmem_limit_bytes=8 * 1024 * 1024),
        )(acc1, acc2)
        return v1.transpose(0, 2, 1), v2

    return jax.shard_map(local_part, mesh=mesh,
                         in_specs=(P(('frag', 'dev')), P('frag'), P('frag')),
                         out_specs=(P('frag', None, 'dev'), P('frag', None, 'dev')),
                         check_vma=False)
```

```python
import functools
import math

import jax
import jax.numpy as jnp
from jax import lax
from jax.experimental import pallas as pl
from jax.experimental.pallas import tpu as pltpu
from jax.sharding import PartitionSpec as P

F32 = jnp.float32
BF16 = jnp.bfloat16
LANES = 128
TILE = 16
GROUP = 8


def _dot(lhs, rhs):
    return lax.dot_general(lhs, rhs, (((1,), (0,)), ((), ())), preferred_element_type=F32)


def _pieces(n_vir, moved):
    spare = LANES - n_vir
    slots = []
    for t in range(-(-moved * n_vir // spare)):
        runs = []
        col, end = t * spare, min((t + 1) * spare, moved * n_vir)
        at = n_vir
        while col < end:
            count = min(end, (col // n_vir + 1) * n_vir) - col
            runs.append((col // n_vir, col % n_vir, at, count))
            col, at = col + count, at + count
        slots.append(runs)
    return slots


def _order(side):
    def hops(d):
        return min(d, side - d)

    left = {(dx, dy) for dx in range(side) for dy in range(side)}
    chips = []
    for dx, dy in sorted(left, key=lambda c: (-(hops(c[0]) > 0) - (hops(c[1]) > 0),
                                              abs(hops(c[0]) - hops(c[1])), hops(c[0]), c)):
        for chip in ((dx, dy), (-dx % side, -dy % side), (dy, -dx % side), (-dy % side, dx)):
            if chip in left:
                left.remove(chip)
                chips.append(chip)
    return [(dx, dy, other) for dx, dy in chips for other in (1, 0)]


def _kernel(n_dev, rows, n_ao, n_occ, n_vir, q_chunk, n_buf, pitch, keep, unroll,
            a_hbm, cot_hbm, cv_hbm, acc1, acc2,
            cot_ref, cv_ref, abuf, tb0, tb1, w2, ct, hov0, hov1, hoo0, hoo1, sb, rb, rep, wk, csem, asem, ssem, rsem):
    me = lax.axis_index('dev')
    hov, hoo = (hov0, hov1), (hoo0, hoo1)
    side = math.isqrt(n_dev // 2)
    core, cx, cy = lax.rem(me, 2), lax.rem(me // 2, side), me // (2 * side)
    order = _order(side)

    def partner(step, away):
        dx, dy, other = order[step]
        there = lax.rem(core + other, 2)
        sign = away * (1 - 2 * (core if away > 0 else there))
        return ((lax.rem(cy + dy * sign + side, side) * side + lax.rem(cx + dx * sign + side, side)) * 2
                + there)

    n_chunk = n_ao // q_chunk
    n_half = n_dev // 2
    total = rows * n_chunk
    moved = (n_occ + n_vir) // GROUP - keep
    slots = _pieces(n_vir, moved)
    block_rows = keep * GROUP
    cuts = (0, 2 * TILE, 4 * TILE, 6 * TILE, block_rows)

    def fetch(chunk):
        slot = lax.rem(chunk, n_buf)
        return pltpu.make_async_copy(
            a_hbm.at[chunk // n_chunk, pl.ds(lax.rem(chunk, n_chunk) * q_chunk, q_chunk)],
            abuf.at[slot], asem.at[slot])

    coefs = (pltpu.make_async_copy(cot_hbm, cot_ref, csem.at[0]),
             pltpu.make_async_copy(cv_hbm, cv_ref, csem.at[1]))
    for copy in coefs:
        copy.start()
    for first in range(n_buf):
        fetch(jnp.int32(first)).start()

    barrier = pltpu.get_barrier_semaphore()

    @pl.loop(1, n_dev)
    def _(k):
        pl.semaphore_signal(barrier, inc=1, device_id={'dev': lax.rem(me + k, n_dev)},
                            device_id_type=pl.DeviceIdType.MESH)

    acc1[...] = jnp.zeros_like(acc1)
    acc2[...] = jnp.zeros_like(acc2)
    w2[...] = jnp.zeros_like(w2)
    for copy in coefs:
        copy.wait()

    w2[:n_ao, :n_vir] = cv_ref[...]
    w2[:n_ao, LANES:LANES + n_occ] = cot_ref[...].astype(F32).T.astype(BF16)
    ct[:n_occ, :] = cot_ref[...]
    ct[n_occ:, :] = cv_ref[...].astype(F32).T.astype(BF16)
    lane = lax.broadcasted_iota(jnp.int32, (GROUP, LANES), 1)

    pl.semaphore_wait(barrier, n_dev - 1)

    def send(row, steps):
        for low, high in zip(cuts, cuts[1:]):
            for step in steps:
                pltpu.make_async_remote_copy(
                    src_ref=sb.at[row, step, low:high], dst_ref=rb.at[row, step, low:high],
                    send_sem=ssem.at[row], recv_sem=rsem.at[row, step // n_half],
                    device_id={'dev': partner(step, 1)}, device_id_type=pl.DeviceIdType.MESH).start()

    @pl.loop(0, rows)
    def _(row):
        @pl.loop(0, n_chunk)
        def _(part):
            chunk = row * n_chunk + part
            slot = lax.rem(chunk, n_buf)
            fetch(chunk).wait()

            for q in range(q_chunk):
                t = _dot(cot_ref[...], abuf[slot, q])
                at = pl.ds(part * q_chunk + q, n_occ, stride=pitch)
                tb0[at, :] = t[:, :LANES]
                tb1[at, :] = jnp.pad(t[:, LANES:], ((0, 0), (0, 2 * LANES - n_ao)))

            @pl.when(chunk + n_buf < total)
            def _():
                fetch(chunk + n_buf).start()

        def half(group):
            parts = []
            for u in range(unroll):
                at = pl.ds(pl.multiple_of(partner(group * unroll + u, 1) * pitch, 8), n_ao)
                parts.append(jnp.concatenate([tb0[at, :].astype(BF16), tb1[at, :].astype(BF16)], axis=1))
            h = _dot(jnp.concatenate(parts, axis=0), w2[...])
            for u in range(unroll):
                at = slice(u * n_ao, (u + 1) * n_ao)
                hov[group % 2][u] = h[at, :LANES].astype(BF16)
                hoo[group % 2][u * n_occ:(u + 1) * n_occ, :] = h[at, LANES:LANES + n_occ].T.astype(BF16)

        def full(group):
            goo = _dot(hoo[group % 2][...], w2[:n_ao, :LANES])
            for u in range(0, unroll, 2):
                pair = _dot(ct[n_occ:, :], jnp.concatenate([hov[group % 2][u], hov[group % 2][u + 1]], axis=1))
                for v in range(2):
                    gov = pair[:, v * LANES:(v + 1) * LANES]
                    first = (u + v) * n_occ
                    groups = [goo[first + g * GROUP:first + (g + 1) * GROUP] for g in range(n_occ // GROUP)]
                    groups += [gov[g * GROUP:(g + 1) * GROUP] for g in range(n_vir // GROUP)]
                    out = []
                    for t_, value in enumerate(groups[:keep]):
                        for part, src, dst, _count in (slots[t_] if t_ < len(slots) else ()):
                            tail = groups[keep + part]
                            if (dst - src) % LANES:
                                tail = pltpu.roll(tail, (dst - src) % LANES, 1)
                            value = jnp.where(lane < dst, value, tail)
                        out.append(value)
                    sb[row, group * unroll + u + v] = jnp.concatenate(out, axis=0).astype(BF16)

        n_group = n_dev // unroll
        half(0)
        for group in range(n_group):
            if group + 1 < n_group:
                half(group + 1)
            full(group)
            first, last = group * unroll, (group + 1) * unroll
            send(row, range(max(first - 2, 0), last - 2))
        rb[row, n_dev - 1] = sb[row, n_dev - 1]
        send(row, [n_dev - 2])

    ident = (lax.broadcasted_iota(jnp.int32, (TILE, n_dev * TILE), 1) % TILE
             == lax.broadcasted_iota(jnp.int32, (TILE, n_dev * TILE), 0))
    slot = lax.broadcasted_iota(jnp.int32, (1, n_dev * TILE), 1) // TILE
    owner = jnp.zeros_like(slot)
    for step in range(n_dev):
        owner = jnp.where(slot == step, partner(step, -1) * rows, owner)
    place = lax.broadcasted_iota(jnp.int32, (n_ao, n_dev * TILE), 0)
    n_tile = block_rows // TILE
    oo_rows = n_occ * TILE

    def weights(row):
        pick = jnp.where(place == owner + row, 1.0, 0.0).astype(BF16)
        rep[...] = _dot(ct[...], pick)

        @pl.loop(0, (n_occ + n_vir) // 8)
        def _(block):
            for u in range(8):
                i = block * 8 + u
                value = jnp.where(ident, rep[pl.ds(i, 1), :], 0.0).astype(BF16)
                wk[pl.ds(pl.multiple_of(i * TILE, TILE), TILE), :] = value

    def arrived(row, part):
        blocks = rb.at[row, pl.ds(part * n_half, n_half - part)]
        pltpu.make_async_copy(blocks, blocks, rsem.at[row, part]).wait()

    def contract(row, low, high):
        cols = slice(low * TILE, high * TILE)

        def tiles(first, count):
            parts = [rb[row, low:high, t * TILE:(t + 1) * TILE, :].reshape((high - low) * TILE, LANES)
                     for t in range(first, first + count)]
            return parts[0] if count == 1 else jnp.concatenate(parts, axis=1)

        for first in range(0, n_tile, 2):
            count = min(2, n_tile - first)
            out = _dot(wk[:oo_rows, cols], tiles(first, count))
            for c in range(count):
                at = slice((first + c) * TILE, (first + c + 1) * TILE)
                acc2[:, at, :] += out[:, c * LANES:(c + 1) * LANES].reshape(n_occ, TILE, LANES)

        n_block = 4
        span = n_vir // n_block
        rhs = tiles(0, n_occ // TILE)

        def part(block):
            at = pl.ds(oo_rows + block * (span * TILE), span * TILE)
            out = _dot(wk[at, cols], rhs)
            for c in range(n_occ // TILE):
                acc1[pl.ds(block * span, span), c * TILE:(c + 1) * TILE, :] += (
                    out[:, c * LANES:c * LANES + n_vir].reshape(span, TILE, n_vir))

        for block in range(n_block):
            part(block)

    @pl.loop(0, rows - 1)
    def _(row):
        weights(row)
        arrived(row, 0)
        arrived(row, 1)
        contract(row, 0, n_dev)

    weights(rows - 1)
    for part in range(2):
        arrived(rows - 1, part)
        contract(rows - 1, part * n_half, (part + 1) * n_half)

    for row in range(rows):
        pltpu.make_async_copy(sb.at[row, pl.ds(0, n_dev - 1)], sb.at[row, pl.ds(0, n_dev - 1)],
                              ssem.at[row]).wait()


def _unpack(n_occ, n_vir, keep, acc1, acc2, v1_ref, v2_ref, v2, sem):
    moved = (n_occ + n_vir) // GROUP - keep
    head = n_vir // GROUP - moved
    slots = _pieces(n_vir, moved)
    lane = lax.broadcasted_iota(jnp.int32, (GROUP, LANES), 1)
    copies = [pltpu.make_async_copy(acc1, v1_ref, sem.at[0])]
    copies[0].start()
    for i in range(n_occ):
        v2[i, :head * GROUP, :] = acc2[i, n_occ:n_occ + head * GROUP, :n_vir]
        for group in range(moved):
            value = None
            for t, runs in enumerate(slots):
                for g, src, dst, _count in runs:
                    if g == group:
                        piece = acc2[i, t * GROUP:(t + 1) * GROUP, :]
                        if (src - dst) % LANES:
                            piece = pltpu.roll(piece, (src - dst) % LANES, 1)
                        value = piece if value is None else jnp.where(lane < src, value, piece)
            v2[i, (head + group) * GROUP:(head + group + 1) * GROUP, :] = value[:, :n_vir]
        if i % 8 == 7:
            at = pl.ds(i - 7, 8)
            copies.append(pltpu.make_async_copy(v2.at[at], v2_ref.at[at], sem.at[1 + i // 8]))
            copies[-1].start()
    for copy in copies:
        copy.wait()


def solution(mesh):
    n_dev = mesh.shape['dev']

    def local_part(ao_rows, c_occ, c_vir):
        rows, n_ao = ao_rows.shape[:2]
        n_occ, n_vir = c_occ.shape[1], c_vir.shape[1]
        assert n_occ == n_dev
        q_chunk, n_buf, pitch = 32, 5, n_ao + 8
        keep, unroll = 14, 8
        block_rows = keep * GROUP
        n_mo = n_occ + n_vir
        acc1, acc2 = pl.pallas_call(
            functools.partial(_kernel, n_dev, rows, n_ao, n_occ, n_vir, q_chunk, n_buf, pitch, keep, unroll),
            out_shape=(pltpu.VMEM((n_vir, n_occ, n_vir), F32),
                       pltpu.VMEM((n_occ, block_rows, LANES), F32)),
            in_specs=[pl.BlockSpec(memory_space=pltpu.HBM)] * 3,
            out_specs=(pl.BlockSpec(memory_space=pltpu.VMEM), pl.BlockSpec(memory_space=pltpu.VMEM)),
            scratch_shapes=[
                pltpu.VMEM((n_occ, n_ao), BF16),
                pltpu.VMEM((n_ao, n_vir), BF16),
                pltpu.VMEM((n_buf, q_chunk, n_ao, n_ao), BF16),
                pltpu.VMEM((n_occ * pitch, LANES), F32),
                pltpu.VMEM((n_occ * pitch, LANES), F32),
                pltpu.VMEM((2 * LANES, 2 * LANES), BF16),
                pltpu.VMEM((n_mo, n_ao), BF16),
                pltpu.VMEM((unroll, n_ao, LANES), BF16),
                pltpu.VMEM((unroll, n_ao, LANES), BF16),
                pltpu.VMEM((unroll * n_occ, n_ao), BF16),
                pltpu.VMEM((unroll * n_occ, n_ao), BF16),
                pltpu.VMEM((rows, n_dev, block_rows, LANES), BF16),
                pltpu.VMEM((rows, n_dev, block_rows, LANES), BF16),
                pltpu.VMEM((n_mo, n_dev * TILE), F32),
                pltpu.VMEM((n_mo * TILE, n_dev * TILE), BF16),
                pltpu.SemaphoreType.DMA((2,)),
                pltpu.SemaphoreType.DMA((n_buf,)),
                pltpu.SemaphoreType.DMA((rows,)),
                pltpu.SemaphoreType.DMA((rows, 2)),
            ],
            compiler_params=pltpu.CompilerParams(collective_id=0, has_side_effects=True,
                                                 vmem_limit_bytes=44 * 1024 * 1024),
        )(ao_rows, *(pltpu.with_memory_space_constraint(c, pltpu.HBM) for c in (c_occ.T, c_vir)))
        v1, v2 = pl.pallas_call(
            functools.partial(_unpack, n_occ, n_vir, keep),
            out_shape=(jax.ShapeDtypeStruct((n_vir, n_occ, n_vir), F32),
                       jax.ShapeDtypeStruct((n_occ, n_vir, n_vir), F32)),
            in_specs=[pl.BlockSpec(memory_space=pltpu.VMEM)] * 2,
            out_specs=(pl.BlockSpec(memory_space=pl.ANY), pl.BlockSpec(memory_space=pl.ANY)),
            scratch_shapes=[pltpu.VMEM((n_occ, n_vir, n_vir), F32), pltpu.SemaphoreType.DMA((1 + n_occ // 8,))],
            compiler_params=pltpu.CompilerParams(vmem_limit_bytes=8 * 1024 * 1024),
        )(acc1, acc2)
        return v1.transpose(0, 2, 1), v2

    return jax.shard_map(local_part, mesh=mesh,
                         in_specs=(P(('frag', 'dev')), P('frag'), P('frag')),
                         out_specs=(P('frag', None, 'dev'), P('frag', None, 'dev')),
                         check_vma=False)
```
